32 devices in a mesh: dp: 4 (over z), expert: 8 (over y, x, core).
Axes of the slice: x: 2, y: 2, z: 4, core: 2. Of those that a mesh axis runs over, the one named last changes fastest.
Arguments:
- grad_output: bfloat16 [8, 8, 3840], P('expert', None, 'dp'), may hold values from -6 to 6
- router_logits: float32 [8, 8, 32], P('expert'), may hold values from -8 to 8
- expert_ids: int32 [8, 8, 8], P('expert'), may hold values from 0 to 31, all different within a row; in each aligned block of 8 rows (0 to 7, 8 to 15, ..., all dimensions but the last counted through in order) at most 3 rows name the same one
- router_input: bfloat16 [8, 8, 3840], P('expert', 'dp'), may hold values from -6 to 6
- router_weight: bfloat16 [32, 3840], P(None, 'dp'), may hold values from -0.09375 to 0.09375
- gate_weight: bfloat16 [32, 3840, 1024], P('expert', 'dp'), may hold values from -0.09375 to 0.09375
- up_weight: bfloat16 [32, 3840, 1024], P('expert', 'dp'), may hold values from -0.09375 to 0.09375
- down_weight: bfloat16 [32, 1024, 3840], P('expert', None, 'dp'), may hold values from -0.1875 to 0.1875
- gate_saved: bfloat16 [32, 24, 1024], P('expert'), may hold values from -6 to 6
- up_saved: bfloat16 [32, 24, 1024], P('expert'), may hold values from -6 to 6
Outputs:
- grad_input: bfloat16 [8, 8, 3840], P('expert', None, 'dp')
- grad_router: float32 [32, 3840], P('expert', 'dp')
The draws below stay inside these ranges and needn't reach their ends.
Inputs may be any that keep to these rules, and one draw needn't show every extreme that they name: `expert_ids`: within one token group (the 8 tokens of one index of expert, in order), no expert is named more than 3 times, a bound that some block reaches; every row names 8 different experts.
All inputs are finite; a program needn't handle non-finite values.
Results may differ from the reference program's by a relative error of at most 0.008.
Values may be sent and summed in bfloat16 or wider, within the bound.
No kernel may reach another device: no remote copies, remote signals or barrier semaphores. Data moves between devices by JAX's collectives and lax.ppermute only.
A program may use at most 64 MiB of HBM per device.

```python
import math
import jax
import jax.numpy as jnp
import numpy as np
from jax import lax

D = 3840
F = 1024
TOP = 8
EXPERTS = 32
GROUP = 8
MOST = 3
SLOTS = 24
N_EXPERT = 8


def level_of(own_key, extent, pieces, smallest, top_value):
    def one(axis_at, parts):
        steps = jax.random.uniform(jax.random.fold_in(jax.random.fold_in(own_key, 6), axis_at), (parts,), jnp.float32, smallest / len(pieces), top_value / len(pieces))
        return jnp.repeat(jnp.exp(steps), extent[axis_at] // parts).reshape((-1,) + (1,) * (len(extent) - axis_at - 1))

    loudness = one(*pieces[0])
    for cut in pieces[1:]:
        loudness = loudness * one(*cut)
    return loudness


def routed_block(stream_key, own, number, rows, count, top, limit, lean):
    order = jax.random.permutation(stream_key, count)
    packed, usual = portions_of(count, rows * top, limit, lean, True), portions_of(count, rows * top, limit, lean, False)
    places = jnp.arange(count)

    def named(tallies, offset_by):
        used = int((tallies > 0).sum())
        fixed = max(1, used // 4)
        shifted = fixed + (places - fixed + offset_by * (used - fixed)) % max(1, count - fixed)
        return jnp.zeros((count,), jnp.int32).at[order[jnp.where(places < fixed, places, shifted)]].set(jnp.asarray(tallies, jnp.int32))

    tallies = jnp.where(number % 4 == 0, named(packed, number // 4), named(usual, number - number // 4 - 1))
    mixed = jax.random.permutation(jax.random.fold_in(own, 3), count)
    donor, sink = mixed[0:count // 2 * 2:2], mixed[1:count // 2 * 2:2]
    slack = jnp.minimum(tallies[donor] - 1, limit - tallies[sink]) // 2
    slack = jnp.where((donor == order[0]) | (sink == order[0]) | (tallies[sink] == 0), 0, jnp.maximum(slack, 0))
    shifted = jax.random.randint(jax.random.fold_in(own, 4), (count // 2,), 0, 1 << 20) % (slack + 1)
    tallies = tallies.at[donor].add(-shifted).at[sink].add(shifted)
    labels = jnp.searchsorted(jnp.cumsum(tallies), jnp.arange(rows * top), side="right").astype(jnp.int32)
    grid = labels.reshape(top, rows).T
    grid = grid[jax.random.permutation(jax.random.fold_in(own, 1), rows)]
    offset_by = jax.random.randint(jax.random.fold_in(own, 2), (rows, 1), 0, top)
    return jnp.take_along_axis(grid, (jnp.arange(top)[None, :] + offset_by) % top, axis=1)


def portions_of(number_of, total, reach, skew, full):
    weights = [(1 << 20) // math.isqrt(rank ** skew) + 1 for rank in range(1, number_of + 1)]
    largest = reach if full else min(reach, max(-(-total // number_of), total * weights[0] // sum(weights)))
    least = 1 if total - largest >= number_of - 1 else 0
    holding, surplus = [largest] + [least] * (number_of - 1), total - largest - least * (number_of - 1)
    while surplus > 0:
        movable = [i for i in range(1, number_of) if holding[i] < largest] or [i for i in range(1, number_of) if holding[i] < reach]
        mass, left = sum([weights[i] for i in movable]), surplus
        for i in movable:
            more = min(reach - holding[i], max(1, left * weights[i] // mass), surplus)
            holding[i] = holding[i] + more
            surplus = surplus - more
    return np.array(holding)


def bell_draw(own_key, dims, width, reach, split=(), held_as=jnp.bfloat16):
    loudness = level_of(own_key, dims, split, -0.22, 0.18) if split else 1.0
    array = jax.random.normal(own_key, dims, jnp.float32) * width * loudness
    return jnp.minimum(jnp.maximum(array, -reach), reach).astype(held_as)


def setup_inputs(seed: int = 0) -> dict:
    seeds = jax.random.split(jax.random.key(seed), 11)
    grad_output = bell_draw(seeds[0], (N_EXPERT, GROUP, D), 1.0, 6.0, ((0, 8), (2, 4)))
    router_logits = bell_draw(seeds[1], (N_EXPERT, GROUP, EXPERTS), 1.5, 8.0, ((0, 8),), jnp.float32)
    expert_ids_keys = jax.random.split(jax.random.fold_in(seeds[2], 1), N_EXPERT * GROUP // GROUP)
    expert_ids_turns = jax.random.permutation(jax.random.fold_in(seeds[2], 3), N_EXPERT * GROUP // GROUP)
    expert_ids = jax.vmap(lambda own, number: routed_block(jax.random.fold_in(seeds[2], 2), own, number, GROUP, EXPERTS, TOP, MOST, 2))(expert_ids_keys, expert_ids_turns).reshape((N_EXPERT, GROUP, TOP))
    router_input = bell_draw(seeds[3], (N_EXPERT, GROUP, D), 1.0, 6.0, ((0, 8), (1, 4)))
    router_weight = bell_draw(seeds[4], (EXPERTS, D), D ** -0.5, 0.09375, ((1, 4),))
    gate_weight = bell_draw(seeds[5], (EXPERTS, D, F), D ** -0.5, 0.09375, ((0, 8), (1, 4)))
    up_weight = bell_draw(seeds[6], (EXPERTS, D, F), D ** -0.5, 0.09375, ((0, 8), (1, 4)))
    down_weight = bell_draw(seeds[7], (EXPERTS, F, D), F ** -0.5, 0.1875, ((0, 8), (2, 4)))
    gate_saved = bell_draw(seeds[8], (EXPERTS, SLOTS, F), 1.0, 6.0, ((0, 8),))
    up_saved = bell_draw(seeds[9], (EXPERTS, SLOTS, F), 1.0, 6.0, ((0, 8),))
    return {"grad_output": grad_output, "router_logits": router_logits, "expert_ids": expert_ids, "router_input": router_input, "router_weight": router_weight, "gate_weight": gate_weight, "up_weight": up_weight, "down_weight": down_weight, "gate_saved": gate_saved, "up_saved": up_saved}


route_scale = 2.5


def expert_backward(operands):
    out_grad, weight_gate, weight_up, weight_down, saved_gate, saved_up = operands
    hidden_grad = jnp.dot(out_grad, weight_down.T, preferred_element_type=jnp.float32)
    gate_value = saved_gate.astype(jnp.float32)
    up_value = saved_up.astype(jnp.float32)
    gate_sigmoid = jax.nn.sigmoid(gate_value)
    activated = gate_value * gate_sigmoid
    hidden = lax.optimization_barrier((activated * up_value).astype(jnp.bfloat16)).astype(jnp.float32)
    gate_grad = jnp.sum(hidden * hidden_grad, axis=1)
    grad_gate = (hidden_grad * up_value * gate_sigmoid * (1.0 + gate_value * (1.0 - gate_sigmoid))).astype(jnp.bfloat16)
    grad_up = (hidden_grad * activated).astype(jnp.bfloat16)
    input_grad = jnp.dot(grad_gate, weight_gate.T, preferred_element_type=jnp.float32)
    input_grad = input_grad + jnp.dot(grad_up, weight_up.T, preferred_element_type=jnp.float32)
    return input_grad.astype(jnp.bfloat16), gate_grad


def reference(grad_output, router_logits, expert_ids, router_input, router_weight, gate_weight, up_weight, down_weight, gate_saved, up_saved):
    assign_count = GROUP * TOP
    flat_ids = expert_ids.reshape(N_EXPERT, assign_count).astype(jnp.int32)
    expert_hot = (flat_ids[:, :, None] == jnp.arange(EXPERTS, dtype=jnp.int32)[None, None, :]).astype(jnp.int32)
    earlier = (jnp.cumsum(expert_hot, axis=1) - expert_hot).astype(jnp.int32)
    ranking = jnp.sum(expert_hot * earlier, axis=2).astype(jnp.int32)
    slot_index = (jnp.arange(N_EXPERT, dtype=jnp.int32)[:, None] * MOST + ranking).astype(jnp.int32)
    owner = (jnp.arange(assign_count, dtype=jnp.int32) // TOP).astype(jnp.int32)
    routed_rows = grad_output[:, owner, :]
    dispatched = jnp.zeros((EXPERTS, SLOTS, D), jnp.bfloat16).at[flat_ids, slot_index].set(routed_rows)
    expert_input, gate_grad = lax.map(expert_backward, (dispatched, gate_weight, up_weight, down_weight, gate_saved, up_saved))
    back_rows = expert_input[flat_ids, slot_index].astype(jnp.float32).reshape(N_EXPERT, GROUP, TOP, D)
    back_gate = gate_grad[flat_ids, slot_index].astype(jnp.float32).reshape(N_EXPERT, GROUP, TOP)
    scores = jax.nn.sigmoid(router_logits)
    chosen = jnp.take_along_axis(scores, expert_ids.astype(jnp.int32), axis=2)
    chosen_total = jnp.sum(chosen, axis=2, keepdims=True)
    gates = route_scale * chosen / chosen_total
    mixed = jnp.sum(gates[:, :, :, None] * back_rows, axis=2)
    mixture = jnp.sum(back_gate * gates, axis=2, keepdims=True)
    d_chosen = (route_scale * back_gate - mixture) / chosen_total
    hot_float = expert_hot.reshape(N_EXPERT, GROUP, TOP, EXPERTS).astype(jnp.float32)
    d_scores = jnp.sum(hot_float * d_chosen[:, :, :, None], axis=2)
    logit_grad = (d_scores * scores * (1.0 - scores)).astype(jnp.bfloat16)
    router_part = jnp.einsum("qge,ed->qgd", logit_grad.astype(jnp.float32), router_weight.astype(jnp.float32))
    grad_input = (mixed + router_part).astype(jnp.bfloat16)
    grad_router = jnp.einsum("qge,qgd->ed", logit_grad.astype(jnp.float32), router_input.astype(jnp.float32))
    return grad_input, grad_router
```

```python
import functools

import jax
import jax.numpy as jnp
from jax import lax
from jax.experimental import pallas as pl
from jax.experimental.pallas import tpu as pltpu
from jax.sharding import PartitionSpec as P

route_scale = 2.5
LANES = 128
HIGH = lax.Precision.HIGHEST
VMEM = pltpu.VMEM


def spec(space):
    return pl.BlockSpec(memory_space=space)


def iota(shape, dim):
    return lax.broadcasted_iota(jnp.int32, shape, dim)


def pairwise(count):
    return count <= 8 and count & (count - 1) == 0


def place_of(block, me, count):
    return lax.bitwise_xor(block, me) if pairwise(count) else block


def pack_kernel(expert_total, logits_ref, ids_ref, rows_ref, out_ref):
    copies, group, width = out_ref.shape
    top = ids_ref.shape[2]
    share = rows_ref.shape[2]
    aux = width - share
    logits = logits_ref[0]
    first = logits.astype(jnp.bfloat16).astype(jnp.float32)
    rest = logits - first
    second = rest.astype(jnp.bfloat16).astype(jnp.float32)
    third = rest - second
    pieces = [first, second, third, ids_ref[0].astype(jnp.float32)]
    spare = aux - 3 * expert_total - top
    if spare:
        pieces.append(jnp.zeros((group, spare), jnp.float32))
    head = jnp.concatenate(pieces, axis=1).astype(jnp.bfloat16)
    rows = rows_ref[0]
    for copy in range(copies):
        out_ref[copy, :, :aux] = head
        out_ref[copy, :, aux:] = rows


def down_kernel(
    sizes, tokens_ref, weight_ref, send_ref, high_ref, low_ref, gates_ref, slope_ref, slot_ref, held, sems
):
    group, expert_total, top, aux, depth, local_experts, slots, dp_count = sizes
    tokens, width = tokens_ref.shape
    rows = local_experts * slots
    piece = rows // dp_count
    per_expert = slots // piece
    copies = [
        pltpu.make_async_copy(weight_ref.at[e], held.at[e], sems.at[e]) for e in range(local_experts)
    ]
    for copy in copies:
        copy.start()
    dp_me = lax.axis_index("dp")
    base = lax.axis_index("expert") * local_experts
    head = tokens_ref[:, :aux].astype(jnp.float32)
    logits = (
        head[:, :expert_total]
        + head[:, expert_total : 2 * expert_total]
        + head[:, 2 * expert_total : 3 * expert_total]
    )
    lane = iota((tokens, expert_total), 1)
    named = jnp.zeros((tokens, expert_total), jnp.float32)
    for k in range(top):
        at = 3 * expert_total + k
        named = named + (head[:, at : at + 1].astype(jnp.int32) == lane).astype(jnp.float32)
    row_at, col_at = iota((tokens, tokens), 0), iota((tokens, tokens), 1)
    earlier = (lax.div(row_at, group) == lax.div(col_at, group)) & (col_at < row_at)
    rank = jnp.dot(
        earlier.astype(jnp.bfloat16), named.astype(jnp.bfloat16), preferred_element_type=jnp.float32
    )
    first_slot = (lax.div(iota((tokens, expert_total), 0), group) * depth).astype(jnp.float32)
    slot = jnp.where(named > 0.5, first_slot + rank, -1.0)
    scores = jax.nn.sigmoid(logits)
    total = jnp.sum(named * scores, axis=1, keepdims=True)
    gates = route_scale * (named * scores) / total
    gates_ref[...] = gates
    slope_ref[...] = named * scores * (1.0 - scores) / total
    slot_ref[...] = slot
    pick = (iota((8, expert_total), 1) == base + iota((8, expert_total), 0)).astype(jnp.float32)
    contract = (((1,), (1,)), ((), ()))
    slot_rows = lax.dot_general(
        pick, slot, contract, precision=HIGH, preferred_element_type=jnp.float32
    )
    spread = (
        iota((expert_total, rows), 0) == base + lax.div(iota((expert_total, rows), 1), slots)
    ).astype(jnp.float32)
    slot_wide = jnp.dot(slot, spread, precision=HIGH, preferred_element_type=jnp.float32)
    gates_wide = jnp.dot(gates, spread, precision=HIGH, preferred_element_type=jnp.float32)
    wanted = lax.rem(iota((tokens, rows), 1), slots).astype(jnp.float32)
    combine = jnp.where(slot_wide == wanted, gates_wide, 0.0)
    upper = combine.astype(jnp.bfloat16)
    high_ref[...] = upper
    low_ref[...] = (combine - upper.astype(jnp.float32)).astype(jnp.bfloat16)
    features = tokens_ref[:, aux:]
    slot_at = iota((slots, tokens), 0).astype(jnp.float32)
    for e in range(local_experts):
        chosen = (slot_at == slot_rows[e : e + 1, :]).astype(jnp.bfloat16)
        sent = jnp.dot(chosen, features, preferred_element_type=jnp.float32).astype(jnp.bfloat16)
        copies[e].wait()
        partial = jnp.dot(sent, held[e], preferred_element_type=jnp.float32)
        for b in range(per_expert):
            send_ref[place_of(e * per_expert + b, dp_me, dp_count)] = partial[
                b * piece : (b + 1) * piece
            ].astype(jnp.bfloat16)


def gathered_blocks(refs):
    if len(refs) == 1 and len(refs[0].shape) == 3:
        return [(refs[0], k) for k in range(refs[0].shape[0])]
    return [(ref, None) for ref in refs]


def read_block(item):
    ref, at = item
    return ref[...] if at is None else ref[at]


def hidden_kernel(block_count, gate_ref, up_ref, *refs):
    parts = gathered_blocks(refs[:block_count])
    hidden_ref, share_ref, gate_held, up_held, sems = refs[block_count:]
    me = lax.axis_index("dp")
    fetches = [
        pltpu.make_async_copy(gate_ref.at[me], gate_held, sems.at[0]),
        pltpu.make_async_copy(up_ref.at[me], up_held, sems.at[1]),
    ]
    for fetch in fetches:
        fetch.start()
    total = read_block(parts[0]).astype(jnp.float32)
    for part in parts[1:]:
        total = total + read_block(part).astype(jnp.float32)
    hidden_ref[...] = total.astype(jnp.bfloat16)
    for fetch in fetches:
        fetch.wait()
    gate_value = gate_held[...].astype(jnp.float32)
    up_value = up_held[...].astype(jnp.float32)
    hidden = (gate_value * jax.nn.sigmoid(gate_value) * up_value).astype(jnp.bfloat16)
    share = jnp.sum(hidden.astype(jnp.float32) * total, axis=1, keepdims=True)
    piece = total.shape[0]
    across = iota((piece, LANES), 0) == iota((piece, LANES), 1)
    line = jnp.sum(jnp.where(across, share, 0.0), axis=0, keepdims=True)
    share_ref[...] = jnp.broadcast_to(line[None], share_ref.shape)


def input_kernel(block_count, slots, gate_w_ref, up_w_ref, high_ref, low_ref, gate_ref, up_ref, *refs):
    parts = gathered_blocks(refs[:block_count])
    out_ref, gate_held, up_held, hidden_held, rows_held, sems = refs[block_count:]
    local_experts = gate_w_ref.shape[0]
    dp_count, piece, _ = hidden_held.shape
    per_expert = slots // piece
    copies = []
    for e in range(local_experts):
        copies.append(pltpu.make_async_copy(gate_w_ref.at[e], gate_held.at[e], sems.at[2 * e]))
        copies.append(pltpu.make_async_copy(up_w_ref.at[e], up_held.at[e], sems.at[2 * e + 1]))
    for copy in copies:
        copy.start()
    me = lax.axis_index("dp")
    for k, part in enumerate(parts):
        hidden_held[place_of(k, me, dp_count)] = read_block(part)
    contract = (((1,), (1,)), ((), ()))
    for e in range(local_experts):
        grads = [
            hidden_held[e * per_expert + b].astype(jnp.float32) for b in range(per_expert)
        ]
        hidden_grad = grads[0] if per_expert == 1 else jnp.concatenate(grads, axis=0)
        gate_value = gate_ref[e].astype(jnp.float32)
        up_value = up_ref[e].astype(jnp.float32)
        sig = jax.nn.sigmoid(gate_value)
        gate_part = (hidden_grad * up_value * sig * (1.0 + gate_value * (1.0 - sig))).astype(jnp.bfloat16)
        up_part = (hidden_grad * (gate_value * sig)).astype(jnp.bfloat16)
        copies[2 * e].wait()
        value = lax.dot_general(gate_part, gate_held[e], contract, preferred_element_type=jnp.float32)
        copies[2 * e + 1].wait()
        value = value + lax.dot_general(
            up_part, up_held[e], contract, preferred_element_type=jnp.float32
        )
        rows_held[e * slots : (e + 1) * slots] = value
    rows = rows_held[...].astype(jnp.bfloat16)
    mixed = jnp.dot(high_ref[...], rows, preferred_element_type=jnp.float32)
    mixed = mixed + jnp.dot(low_ref[...], rows, preferred_element_type=jnp.float32)
    copies_out, group, _ = out_ref.shape
    for q in range(copies_out):
        out_ref[q] = mixed[q * group : (q + 1) * group].astype(jnp.bfloat16)


def router_kernel(
    sizes, shares_ref, gates_ref, slope_ref, slot_ref, inputs_ref, weight_ref, router_ref, part_ref
):
    group, depth, slots, dp_count, expert_count = sizes
    tokens, expert_total = gates_ref.shape
    local_experts = router_ref.shape[0]
    piece = local_experts * slots // dp_count
    per_expert = slots // piece
    devices = dp_count * expert_count
    me = lax.axis_index("expert")
    shares = shares_ref[...].reshape(devices, LANES)
    source = iota((devices, expert_total), 0)
    expert = iota((devices, expert_total), 1)
    dp_of, expert_of = lax.div(source, expert_count), lax.rem(source, expert_count)
    tables = []
    for b in range(per_expert):
        owner = (expert_of == lax.div(expert, local_experts)) & (
            dp_of == lax.rem(expert, local_experts) * per_expert + b
        )
        table = lax.dot_general(
            shares,
            owner.astype(jnp.float32),
            (((0,), (0,)), ((), ())),
            precision=HIGH,
            preferred_element_type=jnp.float32,
        )
        tables.append(table[:piece])
    table = tables[0] if per_expert == 1 else jnp.concatenate(tables, axis=0)
    slot = slot_ref[...]
    first = lax.div(iota((tokens, slots), 0), group) * depth
    column = iota((tokens, slots), 1)
    first_slot = (lax.div(iota((tokens, expert_total), 0), group) * depth).astype(jnp.float32)
    given = jnp.zeros((tokens, expert_total), jnp.float32)
    for r in range(depth):
        line = (column == first + r).astype(jnp.float32)
        found = jnp.dot(line, table, precision=HIGH, preferred_element_type=jnp.float32)
        given = given + jnp.where(slot == first_slot + float(r), found, 0.0)
    mixture = jnp.sum(given * gates_ref[...], axis=1, keepdims=True)
    logit_grad = (slope_ref[...] * (route_scale * given - mixture)).astype(jnp.bfloat16)
    own = (iota((group, tokens), 1) == me * group + iota((group, tokens), 0)).astype(jnp.bfloat16)
    own_grad = jnp.dot(own, logit_grad, preferred_element_type=jnp.float32).astype(jnp.bfloat16)
    part_ref[...] = jnp.dot(own_grad, weight_ref[...], preferred_element_type=jnp.float32)
    pick = (
        iota((8, expert_total), 1) == me * local_experts + iota((8, expert_total), 0)
    ).astype(jnp.bfloat16)
    mine = lax.dot_general(
        pick, logit_grad, (((1,), (1,)), ((), ())), preferred_element_type=jnp.float32
    ).astype(jnp.bfloat16)
    grads = jnp.dot(mine, inputs_ref[...], preferred_element_type=jnp.float32)
    router_ref[...] = grads[:local_experts]


def reduce_blocks(send, count):
    if pairwise(count):
        return [send[0]] + [
            lax.ppermute(send[k], "dp", [(j, j ^ k) for j in range(count)]) for k in range(1, count)
        ]
    return [lax.all_to_all(send, "dp", 0, 0, tiled=True)]


def spread_blocks(block, count):
    if pairwise(count):
        return [block] + [
            lax.ppermute(block, "dp", [(j, j ^ k) for j in range(count)]) for k in range(1, count)
        ]
    return [lax.all_gather(block, "dp", axis=0, tiled=False)]


def local(
    grad_output,
    router_logits,
    expert_ids,
    router_input,
    router_weight,
    gate_weight,
    up_weight,
    down_weight,
    gate_saved,
    up_saved,
):
    expert_count, dp_count = lax.axis_size("expert"), lax.axis_size("dp")
    devices = expert_count * dp_count
    _, group, share = grad_output.shape
    expert_total = router_logits.shape[2]
    top = expert_ids.shape[2]
    local_experts, slots, hidden_size = gate_saved.shape
    depth = slots // expert_count
    rows = local_experts * slots
    piece = rows // dp_count
    tokens = expert_count * group
    aux = -(-(3 * expert_total + top) // LANES) * LANES
    bf16, f32 = jnp.bfloat16, jnp.float32
    shaped = jax.ShapeDtypeStruct

    _, own_tokens, feature_total = router_input.shape
    routed = router_input.reshape(own_tokens, dp_count, share).transpose(1, 0, 2)
    routed = jnp.broadcast_to(routed[:, None], (dp_count, expert_count, own_tokens, share))
    routed = lax.all_to_all(
        routed.reshape(devices, own_tokens, share), ("dp", "expert"), 0, 0, tiled=True
    )
    routed = routed.reshape(dp_count, expert_count, own_tokens, share).transpose(1, 0, 2, 3)
    routed = routed.reshape(tokens, share)

    packed = pl.pallas_call(
        functools.partial(pack_kernel, expert_total),
        out_shape=shaped((expert_count, group, aux + share), bf16),
        in_specs=[spec(VMEM)] * 3,
        out_specs=spec(VMEM),
    )(router_logits, expert_ids, grad_output)
    gathered = lax.all_to_all(packed, "expert", 0, 0, tiled=True).reshape(tokens, aux + share)

    sizes = (group, expert_total, top, aux, depth, local_experts, slots, dp_count)
    table = shaped((tokens, expert_total), f32)
    send, high, low, gates, slope, slot = pl.pallas_call(
        functools.partial(down_kernel, sizes),
        out_shape=(
            shaped((dp_count, piece, hidden_size), bf16),
            shaped((tokens, rows), bf16),
            shaped((tokens, rows), bf16),
            table,
            table,
            table,
        ),
        in_specs=[spec(VMEM), spec(pl.ANY)],
        out_specs=(spec(VMEM),) * 6,
        scratch_shapes=[
            VMEM((local_experts, share, hidden_size), bf16),
            pltpu.SemaphoreType.DMA((local_experts,)),
        ],
    )(gathered, down_weight.swapaxes(1, 2))

    parts = reduce_blocks(send, dp_count)
    hidden, shares = pl.pallas_call(
        functools.partial(hidden_kernel, len(parts)),
        out_shape=(shaped((piece, hidden_size), bf16), shaped((devices, 1, LANES), f32)),
        in_specs=[spec(pl.ANY)] * 2 + [spec(VMEM)] * len(parts),
        out_specs=(spec(VMEM),) * 2,
        scratch_shapes=[
            VMEM((piece, hidden_size), bf16),
            VMEM((piece, hidden_size), bf16),
            pltpu.SemaphoreType.DMA((2,)),
        ],
    )(
        gate_saved.reshape(dp_count, piece, hidden_size),
        up_saved.reshape(dp_count, piece, hidden_size),
        *parts,
    )
    blocks = spread_blocks(hidden, dp_count)
    shares = lax.all_to_all(shares, ("dp", "expert"), 0, 0, tiled=True)

    mixed = pl.pallas_call(
        functools.partial(input_kernel, len(blocks), slots),
        out_shape=shaped((expert_count, group, share), bf16),
        in_specs=[spec(pl.ANY)] * 2 + [spec(VMEM)] * (4 + len(blocks)),
        out_specs=spec(VMEM),
        scratch_shapes=[
            VMEM((local_experts, share, hidden_size), bf16),
            VMEM((local_experts, share, hidden_size), bf16),
            VMEM((dp_count, piece, hidden_size), bf16),
            VMEM((rows, share), f32),
            pltpu.SemaphoreType.DMA((2 * local_experts,)),
        ],
    )(gate_weight, up_weight, high, low, gate_saved, up_saved, *blocks)
    mixed = lax.all_to_all(mixed, "expert", 0, 0, tiled=True)

    grad_router, router_part = pl.pallas_call(
        functools.partial(router_kernel, (group, depth, slots, dp_count, expert_count)),
        out_shape=(shaped((local_experts, share), f32), shaped((group, share), f32)),
        in_specs=[spec(VMEM)] * 6,
        out_specs=(spec(VMEM),) * 2,
    )(shares, gates, slope, slot, routed, router_weight)
    grad_input = jnp.sum(mixed.astype(f32), axis=0) + router_part
    return grad_input.astype(bf16)[None], grad_router


def solution(mesh):
    placed = (
        P("expert", None, "dp"),
        P("expert", None, None),
        P("expert", None, None),
        P("expert", "dp", None),
        P(None, "dp"),
        P("expert", "dp", None),
        P("expert", "dp", None),
        P("expert", None, "dp"),
        P("expert", None, None),
        P("expert", None, None),
    )
    return jax.shard_map(
        local,
        mesh=mesh,
        in_specs=placed,
        out_specs=(P("expert", None, "dp"), P("expert", "dp")),
        check_vma=False,
    )
```

```python
import functools

import jax
import jax.numpy as jnp
from jax import lax
from jax.experimental import pallas as pl
from jax.experimental.pallas import tpu as pltpu
from jax.sharding import PartitionSpec as P

route_scale = 2.5
LANES = 128
HIGH = lax.Precision.HIGHEST
VMEM = pltpu.VMEM
ROWS_ROWS = (((1,), (1,)), ((), ()))


def iota(shape, dim):
    return lax.broadcasted_iota(jnp.int32, shape, dim)


def place_of(block, me, paired):
    return lax.bitwise_xor(block, me) if paired else block


def call(kernel, outs, args, scratch=(), flops=0, far_args=False, far_outs=False):
    far, near = pl.BlockSpec(memory_space=pltpu.HBM), pl.BlockSpec(memory_space=VMEM)
    several = isinstance(outs[0][0], tuple)
    space = pltpu.HBM if far_outs else VMEM
    out_spec = far if far_outs else near
    arg_space = pltpu.HBM if far_args else VMEM
    return pl.pallas_call(
        kernel,
        out_shape=tuple(space(*out) for out in outs) if several else space(*outs),
        in_specs=[far if far_args else near] * len(args),
        out_specs=(out_spec,) * len(outs) if several else out_spec,
        scratch_shapes=list(scratch),
        compiler_params=pltpu.CompilerParams(vmem_limit_bytes=12 << 20),
        cost_estimate=pl.CostEstimate(flops=flops, bytes_accessed=0, transcendentals=0),
    )(*[pltpu.with_memory_space_constraint(arg, arg_space) for arg in args])


def pack_kernel(
    expert_total, logits_far, ids_far, rows_far, out_ref, logits_ref, ids_ref, rows_ref, sems
):
    pairs = ((logits_far, logits_ref), (ids_far, ids_ref), (rows_far, rows_ref))
    fetches = [pltpu.make_async_copy(*pair, sems.at[n]) for n, pair in enumerate(pairs)]
    for fetch in fetches:
        fetch.start()
    for fetch in fetches:
        fetch.wait()
    copies, group, width = out_ref.shape
    top = ids_ref.shape[2]
    aux = width - rows_ref.shape[2]
    logits = logits_ref[0]
    first = logits.astype(jnp.bfloat16).astype(jnp.float32)
    rest = logits - first
    second = rest.astype(jnp.bfloat16).astype(jnp.float32)
    pieces = [first, second, rest - second, ids_ref[0].astype(jnp.float32)]
    spare = aux - 3 * expert_total - top
    if spare:
        pieces.append(jnp.zeros((group, spare), jnp.float32))
    head = jnp.concatenate(pieces, axis=1).astype(jnp.bfloat16)
    rows = rows_ref[0]
    for copy in range(copies):
        out_ref[copy, :, :aux] = head
        out_ref[copy, :, aux:] = rows


def routing(head, sizes):
    group, expert_total, top, depth = sizes
    tokens = head.shape[0]
    lane = iota((tokens, expert_total), 1)
    named = jnp.zeros((tokens, expert_total), jnp.float32)
    for k in range(top):
        at = 3 * expert_total + k
        named = named + (head[:, at : at + 1].astype(jnp.int32) == lane).astype(jnp.float32)
    row_at, col_at = iota((tokens, tokens), 0), iota((tokens, tokens), 1)
    earlier = (lax.div(row_at, group) == lax.div(col_at, group)) & (col_at < row_at)
    rank = jnp.dot(
        earlier.astype(jnp.bfloat16), named.astype(jnp.bfloat16), preferred_element_type=jnp.float32
    )
    first_slot = (lax.div(iota((tokens, expert_total), 0), group) * depth).astype(jnp.float32)
    return named, jnp.where(named > 0.5, first_slot + rank, -1.0)


def down_kernel(sizes, aux, paired, tokens_ref, weight_ref, *send_refs):
    expert_total = sizes[1]
    tokens = tokens_ref.shape[0]
    local_experts = weight_ref.shape[0]
    slots = send_refs[0].shape[0]
    me = lax.axis_index("dp")
    base = lax.axis_index("expert") * local_experts
    _, slot = routing(tokens_ref[:, :aux].astype(jnp.float32), sizes)
    order = place_of(iota((8, expert_total), 0), me, paired)
    pick = (iota((8, expert_total), 1) == base + order).astype(jnp.bfloat16)
    slot_rows = lax.dot_general(
        pick, slot.astype(jnp.bfloat16), ROWS_ROWS, preferred_element_type=jnp.float32
    )
    features = tokens_ref[:, aux:]
    slot_at = iota((slots, tokens), 0).astype(jnp.float32)
    for k, send_ref in enumerate(send_refs):
        chosen = (slot_at == slot_rows[k : k + 1, :]).astype(jnp.bfloat16)
        sent = jnp.dot(chosen, features, preferred_element_type=jnp.float32).astype(jnp.bfloat16)
        weight = weight_ref[place_of(k, me, paired)]
        send_ref[...] = jnp.dot(sent, weight, preferred_element_type=jnp.float32).astype(jnp.bfloat16)


def table_kernel(sizes, local_experts, paired, head_ref, inputs_ref, full_ref, slope_ref, *piece_refs):
    _, expert_total, _, _ = sizes
    tokens, rows = full_ref.shape
    slots = rows // local_experts
    dp_count = lax.axis_size("dp")
    me = lax.axis_index("dp")
    base = lax.axis_index("expert") * local_experts
    head = head_ref[...].astype(jnp.float32)
    logits = (
        head[:, :expert_total]
        + head[:, expert_total : 2 * expert_total]
        + head[:, 2 * expert_total : 3 * expert_total]
    )
    named, slot = routing(head, sizes)
    scores = jax.nn.sigmoid(logits)
    total = jnp.sum(named * scores, axis=1, keepdims=True)
    gates = route_scale * (named * scores) / total
    slope_ref[...] = named * scores * (1.0 - scores) / total
    order = place_of(lax.div(iota((expert_total, rows), 1), slots), me, paired)
    spread = (iota((expert_total, rows), 0) == base + order).astype(jnp.float32)
    slot_wide = jnp.dot(slot, spread, precision=HIGH, preferred_element_type=jnp.float32)
    gates_wide = jnp.dot(gates, spread, precision=HIGH, preferred_element_type=jnp.float32)
    wanted = lax.rem(iota((tokens, rows), 1), slots).astype(jnp.float32)
    full_ref[...] = jnp.where(slot_wide == wanted, gates_wide, 0.0)
    share = inputs_ref.shape[2] // dp_count
    pieces = [inputs_ref[0, :, d * share : (d + 1) * share] for d in range(dp_count)]
    if paired:
        for k, piece_ref in enumerate(piece_refs):
            found = pieces[0]
            for d in range(1, dp_count):
                found = jnp.where(lax.bitwise_xor(k, me) == d, pieces[d], found)
            piece_ref[...] = found
    else:
        for d in range(dp_count):
            piece_refs[0][d] = pieces[d]


def expert_parts(k, paired, gate_w_ref, up_w_ref, gate_ref, up_ref, block_ref, row_ref, share_ref):
    expert = place_of(k, lax.axis_index("dp"), paired)
    hidden_grad = block_ref[...].astype(jnp.float32)
    gate_value = gate_ref[expert].astype(jnp.float32)
    up_value = up_ref[expert].astype(jnp.float32)
    sig = jax.nn.sigmoid(gate_value)
    activated = gate_value * sig
    gate_part = (hidden_grad * up_value * sig * (1.0 + gate_value * (1.0 - sig))).astype(jnp.bfloat16)
    up_part = (hidden_grad * activated).astype(jnp.bfloat16)
    value = lax.dot_general(
        gate_part, gate_w_ref[expert], ROWS_ROWS, preferred_element_type=jnp.float32
    ) + lax.dot_general(up_part, up_w_ref[expert], ROWS_ROWS, preferred_element_type=jnp.float32)
    row_ref[...] = value
    hidden = (activated * up_value).astype(jnp.bfloat16).astype(jnp.float32)
    given = jnp.sum(hidden * hidden_grad, axis=1, keepdims=True)
    slots, width = hidden_grad.shape[0], share_ref.shape[1]
    across = iota((slots, width), 0) + k * slots == iota((slots, width), 1)
    share_ref[...] = jnp.sum(jnp.where(across, given, 0.0), axis=0, keepdims=True)


def input_kernel(k, paired, *refs):
    expert_parts(k, paired, *refs)


def split(values):
    upper = values.astype(jnp.bfloat16)
    return upper, (values - upper.astype(jnp.float32)).astype(jnp.bfloat16)


def mix_kernel(k, paired, piece_count, full_ref, *refs):
    weights, rest = refs[:5], refs[5:]
    piece_refs, rest = rest[:piece_count], rest[piece_count:]
    earlier, (out_ref, own_ref, held_ref, share_ref) = rest[:-4], rest[-4:]
    slots = weights[4].shape[0]
    expert_parts(k, paired, *weights, held_ref.at[pl.ds(k * slots, slots)], share_ref)
    shares = share_ref[...]
    for at in range(k):
        held_ref[at * slots : (at + 1) * slots] = earlier[2 * at][...]
        shares = shares + earlier[2 * at + 1][...]
    full = full_ref[...]
    tokens, rows = full.shape
    local_experts = k + 1
    copies, double, width = out_ref.shape
    group = double // 2
    share = held_ref.shape[1]
    high, low = split(full)
    given = shares[:, :rows]
    mixture = jnp.sum(full * given, axis=1, keepdims=True)
    held_lane = jnp.where(full != 0.0, given, 0.0)
    expert_of = lax.div(iota((tokens, rows), 1), slots)
    own = jnp.zeros((tokens, LANES), jnp.float32)
    for e in range(local_experts):
        dg = jnp.sum(jnp.where(expert_of == e, held_lane, 0.0), axis=1, keepdims=True)
        own = own + jnp.where(iota((tokens, LANES), 1) == e, dg, 0.0)
    own_ref[...] = own
    row_group = lax.div(iota((tokens, LANES), 0), group)
    spread = jnp.where(row_group == iota((tokens, LANES), 1), mixture, 0.0)
    mix_high, mix_low = split(spread)
    same = lax.rem(iota((tokens, tokens), 0), group) == lax.rem(iota((tokens, tokens), 1), group)
    same = same.astype(jnp.bfloat16)
    mix_high = jnp.dot(same, mix_high, preferred_element_type=jnp.float32)
    mix_low = jnp.dot(same, mix_low, preferred_element_type=jnp.float32)
    own_high, own_low = split(own)
    extra = jnp.concatenate(
        [
            mix_high[:, :copies],
            mix_low[:, :copies],
            own_high[:, :local_experts].astype(jnp.float32),
            own_low[:, :local_experts].astype(jnp.float32),
            jnp.zeros((tokens, width - share - 2 * copies - 2 * local_experts), jnp.float32),
        ],
        axis=1,
    ).astype(jnp.bfloat16)
    values = held_ref[...].astype(jnp.bfloat16)
    mixed = jnp.dot(high, values, preferred_element_type=jnp.float32)
    mixed = mixed + jnp.dot(low, values, preferred_element_type=jnp.float32)
    if piece_count == 1:
        routed = piece_refs[0][...].reshape(group, share)
    else:
        routed = jnp.concatenate([ref[...].astype(jnp.float32) for ref in piece_refs], axis=0)
        routed = routed.astype(jnp.bfloat16)
    for q in range(copies):
        lines = slice(q * group, (q + 1) * group)
        out_ref[q, :group, :share] = mixed[lines].astype(jnp.bfloat16)
        out_ref[q, :group, share:] = extra[lines]
        out_ref[q, group:, :share] = routed
        out_ref[q, group:, share:] = jnp.zeros((group, width - share), jnp.bfloat16)


def final_kernel(
    sizes,
    paired,
    got_ref,
    own_ref,
    slope_ref,
    weight_ref,
    input_far,
    router_far,
    input_ref,
    router_ref,
    sems,
):
    group, expert_total, _, _ = sizes
    tokens = slope_ref.shape[0]
    copies = got_ref.shape[0]
    local_experts, share = router_ref.shape
    dp_count = lax.axis_size("dp")
    dp_me, me = lax.axis_index("dp"), lax.axis_index("expert")
    mixed = jnp.zeros((group, share), jnp.float32)
    sums = jnp.zeros((group, 2 * copies), jnp.float32)
    given = jnp.zeros((group, expert_total), jnp.float32)
    own_at = share + 2 * copies
    own_end = own_at + 2 * local_experts
    part = (2 * local_experts, expert_total)
    order = place_of(lax.rem(iota(part, 0), local_experts), dp_me, paired)
    for j in range(copies):
        mixed = mixed + got_ref[j, :group, :share].astype(jnp.float32)
        tail = got_ref[j, :group, share:]
        sums = sums + tail[:, : 2 * copies].astype(jnp.float32)
        to_expert = (iota(part, 1) == j * local_experts + order).astype(jnp.bfloat16)
        given = given + jnp.dot(
            tail[:, 2 * copies : own_end - share], to_expert, preferred_element_type=jnp.float32
        )
    mixture = sums[:, :copies] + sums[:, copies:]
    choose = (iota((tokens, group), 1) == lax.rem(iota((tokens, group), 0), group)).astype(jnp.float32)
    wide = jnp.dot(choose, mixture, precision=HIGH, preferred_element_type=jnp.float32)
    own_group = lax.div(iota((tokens, copies), 0), group) == iota((tokens, copies), 1)
    all_mixture = jnp.sum(jnp.where(own_group, wide, 0.0), axis=1, keepdims=True)
    my_mixture = jnp.sum(
        jnp.where(iota((group, copies), 1) == me, mixture, 0.0), axis=1, keepdims=True
    )
    slope = slope_ref[...]
    my_slope = slope_ref[pl.ds(pl.multiple_of(me * group, group), group), :]
    my_grad = (my_slope * (route_scale * given - my_mixture)).astype(jnp.bfloat16)
    routed = jnp.dot(my_grad, weight_ref[...], preferred_element_type=jnp.float32)
    input_ref[0] = (mixed + routed).astype(jnp.bfloat16)
    store = pltpu.make_async_copy(input_ref, input_far, sems.at[0])
    store.start()
    part = (LANES, expert_total)
    order = place_of(iota(part, 0), dp_me, paired)
    to_expert = (
        (iota(part, 1) == me * local_experts + order) & (iota(part, 0) < local_experts)
    ).astype(jnp.float32)
    mine = jnp.dot(own_ref[...], to_expert, precision=HIGH, preferred_element_type=jnp.float32)
    grads = (slope * (route_scale * mine - all_mixture)).astype(jnp.bfloat16)
    pick = (
        iota((8, expert_total), 1) == me * local_experts + iota((8, expert_total), 0)
    ).astype(jnp.bfloat16)
    lines = lax.dot_general(pick, grads, ROWS_ROWS, preferred_element_type=jnp.float32)
    row, token = iota((tokens, tokens), 1), iota((tokens, tokens), 0)
    own_tokens = group // dp_count
    within = lax.rem(row, group)
    source = lax.div(row, group) * group + (
        place_of(lax.div(within, own_tokens), dp_me, paired) * own_tokens
    ) + lax.rem(within, own_tokens)
    lines = jnp.dot(
        lines.astype(jnp.bfloat16),
        (token == source).astype(jnp.bfloat16),
        preferred_element_type=jnp.float32,
    ).astype(jnp.bfloat16)
    inputs = jnp.concatenate(
        [got_ref[j, group:, :share].astype(jnp.float32) for j in range(copies)], axis=0
    ).astype(jnp.bfloat16)
    router_ref[...] = jnp.dot(lines, inputs, preferred_element_type=jnp.float32)[:local_experts]
    last = pltpu.make_async_copy(router_ref, router_far, sems.at[1])
    last.start()
    store.wait()
    last.wait()


def local(
    grad_output,
    router_logits,
    expert_ids,
    router_input,
    router_weight,
    gate_weight,
    up_weight,
    down_weight,
    gate_saved,
    up_saved,
):
    expert_count, dp_count = lax.axis_size("expert"), lax.axis_size("dp")
    _, group, share = grad_output.shape
    expert_total = router_logits.shape[2]
    top = expert_ids.shape[2]
    local_experts, slots, hidden_size = gate_saved.shape
    depth = slots // expert_count
    rows = local_experts * slots
    piece = rows // dp_count
    tokens = expert_count * group
    aux = -(-(3 * expert_total + top) // LANES) * LANES
    bf16, f32 = jnp.bfloat16, jnp.float32
    paired = dp_count == local_experts and dp_count & (dp_count - 1) == 0
    sizes = (group, expert_total, top, depth)
    swaps = [[(j, j ^ k) for j in range(dp_count)] for k in range(dp_count)]

    packed = call(
        functools.partial(pack_kernel, expert_total),
        ((expert_count, group, aux + share), bf16),
        (router_logits, expert_ids, grad_output),
        scratch=(
            VMEM(router_logits.shape, f32),
            VMEM(expert_ids.shape, jnp.int32),
            VMEM(grad_output.shape, bf16),
            pltpu.SemaphoreType.DMA((3,)),
        ),
        flops=4 * 10**10,
        far_args=True,
    )
    gathered = lax.all_to_all(packed, "expert", 0, 0, tiled=True).reshape(tokens, aux + share)
    sends = call(
        functools.partial(down_kernel, sizes, aux, paired),
        (((slots, hidden_size), bf16),) * local_experts,
        (gathered, down_weight.swapaxes(1, 2)),
    )
    if paired:
        parts = [sends[0]]
        for k in range(1, dp_count):
            parts.append(lax.ppermute(sends[k], "dp", swaps[k]))
    else:
        stacked = jnp.concatenate(sends, axis=0).reshape(dp_count, piece, hidden_size)
        parts = list(lax.all_to_all(stacked, "dp", 0, 0, tiled=True))
    own_tokens = router_input.shape[1]
    if paired:
        piece_shapes = (((own_tokens, share), bf16),) * dp_count
    else:
        piece_shapes = (((dp_count, own_tokens, share), bf16),)
    full, slope, *pieces = call(
        functools.partial(table_kernel, sizes, local_experts, paired),
        (((tokens, rows), f32), ((tokens, expert_total), f32), *piece_shapes),
        (gathered[:, :aux], router_input),
    )
    if paired:
        for k in range(1, dp_count):
            pieces[k] = lax.ppermute(pieces[k], "dp", swaps[k])
    else:
        pieces = [lax.all_to_all(pieces[0], "dp", 0, 0, tiled=True)]

    hidden = sum(part.astype(f32) for part in parts).astype(bf16)
    if paired:
        blocks = [hidden]
        for k in range(1, dp_count):
            blocks.append(lax.ppermute(hidden, "dp", swaps[k]))
    else:
        spread = lax.all_gather(hidden, "dp", axis=0, tiled=True)
        blocks = list(spread.reshape(local_experts, slots, hidden_size))

    weights = (gate_weight, up_weight, gate_saved, up_saved)
    lanes = -(-rows // LANES) * LANES
    done = []
    for k in range(local_experts - 1):
        done += call(
            functools.partial(input_kernel, k, paired),
            (((slots, share), f32), ((1, lanes), f32)),
            (*weights, blocks[k]),
        )
    extra = 2 * expert_count + 2 * local_experts
    width = -(-(share + extra) // LANES) * LANES
    mixed, own = call(
        functools.partial(mix_kernel, local_experts - 1, paired, len(pieces)),
        (((expert_count, 2 * group, width), bf16), ((tokens, LANES), f32)),
        (full, *weights, blocks[-1], *pieces, *done),
        scratch=(VMEM((rows, share), f32), VMEM((1, lanes), f32)),
    )
    got = lax.all_to_all(mixed, "expert", 0, 0, tiled=True)
    grad_input, grad_router = call(
        functools.partial(final_kernel, sizes, paired),
        (((1, group, share), bf16), ((local_experts, share), f32)),
        (got, own, slope, router_weight),
        scratch=(
            VMEM((1, group, share), bf16),
            VMEM((local_experts, share), f32),
            pltpu.SemaphoreType.DMA((2,)),
        ),
        far_outs=True,
    )
    return grad_input, grad_router


def solution(mesh):
    placed = (
        P("expert", None, "dp"),
        P("expert", None, None),
        P("expert", None, None),
        P("expert", "dp", None),
        P(None, "dp"),
        P("expert", "dp", None),
        P("expert", "dp", None),
        P("expert", None, "dp"),
        P("expert", None, None),
        P("expert", None, None),
    )

    return jax.shard_map(
        local,
        mesh=mesh,
        in_specs=placed,
        out_specs=(P("expert", None, "dp"), P("expert", "dp")),
        check_vma=False,
    )
```

```python
import functools

import jax
import jax.numpy as jnp
from jax import lax
from jax.experimental import pallas as pl
from jax.experimental.pallas import tpu as pltpu
from jax.sharding import PartitionSpec as P

route_scale = 2.5
LANES = 128
HIGH = lax.Precision.HIGHEST
VMEM = pltpu.VMEM
ROWS_ROWS = (((1,), (1,)), ((), ()))


def iota(shape, dim):
    return lax.broadcasted_iota(jnp.int32, shape, dim)


def place_of(block, me, paired):
    return lax.bitwise_xor(block, me) if paired else block


def call(kernel, outs, args, scratch=(), flops=0, far_args=False, far_outs=False):
    far, near = pl.BlockSpec(memory_space=pltpu.HBM), pl.BlockSpec(memory_space=VMEM)
    several = isinstance(outs[0][0], tuple)
    space = pltpu.HBM if far_outs else VMEM
    out_spec = far if far_outs else near
    arg_space = pltpu.HBM if far_args else VMEM
    return pl.pallas_call(
        kernel,
        out_shape=tuple(space(*out) for out in outs) if several else space(*outs),
        in_specs=[far if far_args else near] * len(args),
        out_specs=(out_spec,) * len(outs) if several else out_spec,
        scratch_shapes=list(scratch),
        compiler_params=pltpu.CompilerParams(vmem_limit_bytes=12 << 20),
        cost_estimate=pl.CostEstimate(flops=flops, bytes_accessed=0, transcendentals=0),
    )(*[pltpu.with_memory_space_constraint(arg, arg_space) for arg in args])


def group_of(block, count, cubed):
    if not cubed:
        return block
    doubled = 2 * block
    return lax.bitwise_xor(
        lax.rem(doubled, count) + lax.div(doubled, count), lax.axis_index("expert")
    )


def stacked(refs, columns):
    if len(refs) == 1:
        return refs[0][:, columns]
    parts = [ref[:, columns].astype(jnp.float32) for ref in refs]
    return jnp.concatenate(parts, axis=0).astype(refs[0].dtype)


def split(values):
    upper = values.astype(jnp.bfloat16)
    return upper, (values - upper.astype(jnp.float32)).astype(jnp.bfloat16)


def pack_kernel(expert_total, *refs):
    far, out_ref, held, sems = refs[:3], refs[3], refs[4:7], refs[7]
    fetches = [pltpu.make_async_copy(*pair, sems.at[n]) for n, pair in enumerate(zip(far, held))]
    for fetch in fetches:
        fetch.start()
    for fetch in fetches:
        fetch.wait()
    logits_ref, ids_ref, rows_ref = held
    group, width = out_ref.shape
    top = ids_ref.shape[2]
    aux = width - rows_ref.shape[2]
    logits = logits_ref[0]
    first = logits.astype(jnp.bfloat16).astype(jnp.float32)
    rest = logits - first
    second = rest.astype(jnp.bfloat16).astype(jnp.float32)
    pieces = [first, second, rest - second, ids_ref[0].astype(jnp.float32)]
    spare = aux - 3 * expert_total - top
    if spare:
        pieces.append(jnp.zeros((group, spare), jnp.float32))
    out_ref[:, :aux] = jnp.concatenate(pieces, axis=1).astype(jnp.bfloat16)
    out_ref[:, aux:] = rows_ref[0]


def routing(head, sizes, cubed):
    group, expert_total, top, depth = sizes
    tokens = head.shape[0]
    lane = iota((tokens, expert_total), 1)
    named = jnp.zeros((tokens, expert_total), jnp.float32)
    for k in range(top):
        at = 3 * expert_total + k
        named = named + (head[:, at : at + 1].astype(jnp.int32) == lane).astype(jnp.float32)
    row_at, col_at = iota((tokens, tokens), 0), iota((tokens, tokens), 1)
    earlier = (lax.div(row_at, group) == lax.div(col_at, group)) & (col_at < row_at)
    rank = jnp.dot(
        earlier.astype(jnp.bfloat16), named.astype(jnp.bfloat16), preferred_element_type=jnp.float32
    )
    block = lax.div(iota((tokens, expert_total), 0), group)
    first_slot = (group_of(block, tokens // group, cubed) * depth).astype(jnp.float32)
    return named, jnp.where(named > 0.5, first_slot + rank, -1.0)


def down_kernel(sizes, aux, paired, cubed, token_count, *refs):
    token_refs, weight_ref, send_refs = refs[:token_count], refs[token_count], refs[token_count + 1 :]
    expert_total = sizes[1]
    local_experts, share, _ = weight_ref.shape
    slots = send_refs[0].shape[0]
    me = lax.axis_index("dp")
    base = lax.axis_index("expert") * local_experts
    features = stacked(token_refs, slice(aux, aux + share))
    tokens = features.shape[0]
    early = tokens <= 256
    _, slot = routing(stacked(token_refs, slice(0, aux)).astype(jnp.float32), sizes, cubed)
    order = place_of(iota((8, expert_total), 0), me, paired)
    pick = (iota((8, expert_total), 1) == base + order).astype(jnp.bfloat16)
    slot_rows = lax.dot_general(
        pick, slot.astype(jnp.bfloat16), ROWS_ROWS, preferred_element_type=jnp.float32
    )
    slot_at = iota((slots, tokens), 0).astype(jnp.float32)
    for k, send_ref in enumerate(send_refs):
        chosen = (slot_at == slot_rows[k : k + 1, :]).astype(jnp.bfloat16)
        weight = weight_ref[place_of(k, me, paired)]
        if early:
            product = jnp.dot(features, weight, preferred_element_type=jnp.float32)
            value = jnp.dot(chosen, product.astype(jnp.bfloat16), preferred_element_type=jnp.float32)
        else:
            sent = jnp.dot(chosen, features, preferred_element_type=jnp.float32).astype(jnp.bfloat16)
            value = jnp.dot(sent, weight, preferred_element_type=jnp.float32)
        send_ref[...] = value.astype(jnp.bfloat16)


def table_kernel(sizes, aux, local_experts, paired, cubed, token_count, input_count, *refs):
    token_refs, refs = refs[:token_count], refs[token_count:]
    input_refs, (full_ref, slope_ref, *piece_refs) = refs[:input_count], refs[input_count:]
    expert_total = sizes[1]
    tokens, rows = full_ref.shape
    slots = rows // local_experts
    me = lax.axis_index("dp")
    base = lax.axis_index("expert") * local_experts
    head = stacked(token_refs, slice(0, aux)).astype(jnp.float32)
    logits = (
        head[:, :expert_total]
        + head[:, expert_total : 2 * expert_total]
        + head[:, 2 * expert_total : 3 * expert_total]
    )
    named, slot = routing(head, sizes, cubed)
    scores = jax.nn.sigmoid(logits)
    total = jnp.sum(named * scores, axis=1, keepdims=True)
    gates = route_scale * (named * scores) / total
    slope_ref[...] = named * scores * (1.0 - scores) / total
    order = place_of(lax.div(iota((expert_total, rows), 1), slots), me, paired)
    spread = (iota((expert_total, rows), 0) == base + order).astype(jnp.float32)
    slot_wide = jnp.dot(slot, spread, precision=HIGH, preferred_element_type=jnp.float32)
    gates_wide = jnp.dot(gates, spread, precision=HIGH, preferred_element_type=jnp.float32)
    wanted = lax.rem(iota((tokens, rows), 1), slots).astype(jnp.float32)
    full_ref[...] = jnp.where(slot_wide == wanted, gates_wide, 0.0)
    dp_count = lax.axis_size("dp")
    raw = [ref[0] for ref in input_refs]
    share = raw[0].shape[1] // dp_count
    if not cubed:
        for d in range(dp_count):
            piece_refs[0][d] = raw[0][:, d * share : (d + 1) * share]
        return
    both = jnp.concatenate([value.astype(jnp.float32) for value in raw], axis=0)
    lines = [both[:, d * share : (d + 1) * share] for d in range(dp_count)]
    for k, piece_ref in enumerate(piece_refs):
        found = lines[0]
        for d in range(1, dp_count):
            found = jnp.where(place_of(k, me, paired) == d, lines[d], found)
        piece_ref[...] = found.astype(jnp.bfloat16)


def expert_parts(k, paired, gate_w_ref, up_w_ref, gate_ref, up_ref, block_ref, row_ref, share_ref):
    expert = place_of(k, lax.axis_index("dp"), paired)
    hidden_grad = block_ref[...].astype(jnp.float32)
    gate_value = gate_ref[expert].astype(jnp.float32)
    up_value = up_ref[expert].astype(jnp.float32)
    sig = jax.nn.sigmoid(gate_value)
    activated = gate_value * sig
    gate_part = (hidden_grad * up_value * sig * (1.0 + gate_value * (1.0 - sig))).astype(jnp.bfloat16)
    up_part = (hidden_grad * activated).astype(jnp.bfloat16)
    value = lax.dot_general(
        gate_part, gate_w_ref[expert], ROWS_ROWS, preferred_element_type=jnp.float32
    ) + lax.dot_general(up_part, up_w_ref[expert], ROWS_ROWS, preferred_element_type=jnp.float32)
    row_ref[...] = value
    hidden = (activated * up_value).astype(jnp.bfloat16).astype(jnp.float32)
    given = jnp.sum(hidden * hidden_grad, axis=1, keepdims=True)
    slots, width = hidden_grad.shape[0], share_ref.shape[1]
    across = iota((slots, width), 0) + k * slots == iota((slots, width), 1)
    share_ref[...] = jnp.sum(jnp.where(across, given, 0.0), axis=0, keepdims=True)


def input_kernel(k, paired, *refs):
    expert_parts(k, paired, *refs)


def mix_kernel(k, group, paired, cubed, full_ref, *refs):
    weights, rest = refs[:5], refs[5:]
    earlier, out_refs, (held_ref, share_ref) = rest[: 2 * k], rest[2 * k : -2], rest[-2:]
    slots = weights[4].shape[0]
    expert_parts(k, paired, *weights, held_ref.at[pl.ds(k * slots, slots)], share_ref)
    shares = share_ref[...]
    for at in range(k):
        held_ref[at * slots : (at + 1) * slots] = earlier[2 * at][...]
        shares = shares + earlier[2 * at + 1][...]
    full = full_ref[...]
    tokens, rows = full.shape
    local_experts = k + 1
    count = tokens // group
    share, width = held_ref.shape[1], out_refs[0].shape[2]
    given = shares[:, :rows]
    mixture = jnp.sum(full * given, axis=1, keepdims=True)
    held_lane = jnp.where(full != 0.0, given, 0.0)
    expert_at = lax.div(iota((tokens, rows), 1), slots)
    lane = iota((tokens, LANES), 1)
    own = jnp.zeros((tokens, LANES), jnp.float32)
    for e in range(local_experts):
        dg = jnp.sum(jnp.where(expert_at == e, held_lane, 0.0), axis=1, keepdims=True)
        own = own + jnp.where(lane == e, dg, 0.0)
    own_ref = out_refs[-1]
    own_ref[...] = own
    first_core = lax.rem(lax.axis_index("expert"), 2) == 0
    few = own[:, :local_experts]
    none = jnp.zeros_like(few)
    both = jnp.concatenate([jnp.where(first_core, few, none), jnp.where(first_core, none, few)], axis=1)
    row_group = group_of(lax.div(iota((tokens, count), 0), group), count, cubed)
    spread = jnp.where(row_group == iota((tokens, count), 1), mixture, 0.0)
    same = lax.rem(iota((tokens, tokens), 0), group) == lax.rem(iota((tokens, tokens), 1), group)
    same = same.astype(jnp.bfloat16)
    mix_high, mix_low = [
        jnp.dot(same, part, preferred_element_type=jnp.float32) for part in split(spread)
    ]
    own_high, own_low = [part.astype(jnp.float32) for part in split(both)]
    spare = jnp.zeros((tokens, width - share - 2 * count - 4 * local_experts), jnp.float32)
    extra = jnp.concatenate([mix_high, mix_low, own_high, own_low, spare], axis=1)
    values = held_ref[...].astype(jnp.bfloat16)
    high, low = split(full)
    mixed = jnp.dot(high, values, preferred_element_type=jnp.float32)
    mixed = mixed + jnp.dot(low, values, preferred_element_type=jnp.float32)
    at = 0
    for out_ref in out_refs[:-1]:
        for q in range(out_ref.shape[0]):
            lines = slice(at * group, (at + 1) * group)
            out_ref[q, :, :share] = mixed[lines].astype(out_ref.dtype)
            out_ref[q, :, share:] = extra[lines].astype(out_ref.dtype)
            at = at + 1


def pair_kernel(share, count, local_experts, near_ref, far_ref, *refs):
    piece_refs, out_refs = refs[: -near_ref.shape[0]], refs[-near_ref.shape[0] :]
    group, width = near_ref.shape[1:]
    own = group // len(piece_refs)
    pieces = [ref[...].astype(jnp.float32) for ref in piece_refs]
    routed = jnp.concatenate([p[:own] for p in pieces] + [p[own:] for p in pieces], axis=0)
    routed = routed.astype(jnp.bfloat16)
    ends = (0, count, 2 * count, 2 * count + 2 * local_experts, 2 * count + 4 * local_experts)
    for q, out_ref in enumerate(out_refs):
        total = near_ref[q] + far_ref[q].astype(jnp.float32)
        out_ref[:group, :share] = total[:, :share].astype(jnp.bfloat16)
        tail = total[:, share:]
        terms = [tail[:, i:j] for i, j in zip(ends, ends[1:])]
        sums = [terms[0] + terms[1], terms[2] + terms[3]]
        parts = [part.astype(jnp.float32) for value in sums for part in split(value)]
        parts.append(jnp.zeros((group, width - share - ends[-1]), jnp.float32))
        out_ref[:group, share:] = jnp.concatenate(parts, axis=1).astype(jnp.bfloat16)
        out_ref[group:, :share] = routed
        out_ref[group:, share:] = jnp.zeros((2 * group, width - share), jnp.bfloat16)


def final_kernel(sizes, paired, cubed, got_count, input_count, local_experts, *refs):
    got_refs, rest = refs[:got_count], refs[got_count:]
    input_refs, rest = rest[:input_count], rest[input_count:]
    own_ref, slope_ref, weight_ref, input_far, router_far, input_ref, router_ref, sems = rest
    group, expert_total, _, _ = sizes
    tokens = slope_ref.shape[0]
    count = tokens // group
    share = router_ref.shape[1]
    dp_count = lax.axis_size("dp")
    dp_me, me = lax.axis_index("dp"), lax.axis_index("expert")
    if cubed:
        sources = [(ref[:group], lax.bitwise_xor(me, 2 * b)) for b, ref in enumerate(got_refs)]
    else:
        sources = [(got_refs[0][j], j) for j in range(count)]
    mixed = jnp.zeros((group, share), jnp.float32)
    sums = jnp.zeros((group, 2 * count), jnp.float32)
    given = jnp.zeros((group, expert_total), jnp.float32)
    part = (4 * local_experts, expert_total)
    place = lax.rem(iota(part, 0), 2 * local_experts)
    order = place_of(lax.rem(place, local_experts), dp_me, paired)
    for got, source in sources:
        mixed = mixed + got[:, :share].astype(jnp.float32)
        sums = sums + got[:, share : share + 2 * count].astype(jnp.float32)
        first = (source - lax.rem(source, 2) + lax.div(place, local_experts)) * local_experts
        to_expert = (iota(part, 1) == first + order).astype(jnp.bfloat16)
        shares = got[:, share + 2 * count : share + 2 * count + 4 * local_experts]
        given = given + jnp.dot(shares, to_expert, preferred_element_type=jnp.float32)
    mixture = sums[:, :count] + sums[:, count:]
    choose = (iota((tokens, group), 1) == lax.rem(iota((tokens, group), 0), group)).astype(jnp.float32)
    wide = jnp.dot(choose, mixture, precision=HIGH, preferred_element_type=jnp.float32)
    row_group = group_of(lax.div(iota((tokens, count), 0), group), count, cubed)
    all_mixture = jnp.sum(
        jnp.where(row_group == iota((tokens, count), 1), wide, 0.0), axis=1, keepdims=True
    )
    my_mixture = jnp.sum(
        jnp.where(iota((group, count), 1) == me, mixture, 0.0), axis=1, keepdims=True
    )
    slope = slope_ref[...]
    if cubed:
        my_slope = slope[:group]
    else:
        my_slope = slope_ref[pl.ds(pl.multiple_of(me * group, group), group), :]
    my_grad = (my_slope * (route_scale * given - my_mixture)).astype(jnp.bfloat16)
    routed = jnp.dot(my_grad, weight_ref[...], preferred_element_type=jnp.float32)
    input_ref[0] = (mixed + routed).astype(jnp.bfloat16)
    store = pltpu.make_async_copy(input_ref, input_far, sems.at[0])
    store.start()
    part = (LANES, expert_total)
    order = place_of(iota(part, 0), dp_me, paired)
    to_expert = (
        (iota(part, 1) == me * local_experts + order) & (iota(part, 0) < local_experts)
    ).astype(jnp.float32)
    mine = jnp.dot(own_ref[...], to_expert, precision=HIGH, preferred_element_type=jnp.float32)
    grads = (slope * (route_scale * mine - all_mixture)).astype(jnp.bfloat16)
    pick = (
        iota((8, expert_total), 1) == me * local_experts + iota((8, expert_total), 0)
    ).astype(jnp.bfloat16)
    lines = lax.dot_general(pick, grads, ROWS_ROWS, preferred_element_type=jnp.float32)
    row, token = iota((tokens, tokens), 1), iota((tokens, tokens), 0)
    own_tokens = group // dp_count
    within = lax.rem(row, group)
    source = lax.div(row, group) * group + (
        place_of(lax.div(within, own_tokens), dp_me, paired) * own_tokens
    ) + lax.rem(within, own_tokens)
    lines = jnp.dot(
        lines.astype(jnp.bfloat16),
        (token == source).astype(jnp.bfloat16),
        preferred_element_type=jnp.float32,
    ).astype(jnp.bfloat16)
    if cubed:
        parts = [
            ref[half * group : (half + 1) * group, :share].astype(jnp.float32)
            for half in (1, 2)
            for ref in got_refs
        ]
        inputs = jnp.concatenate(parts, axis=0).astype(jnp.bfloat16)
    else:
        inputs = input_refs[0][...]
    router_ref[...] = jnp.dot(lines, inputs, preferred_element_type=jnp.float32)[:local_experts]
    last = pltpu.make_async_copy(router_ref, router_far, sems.at[1])
    last.start()
    store.wait()
    last.wait()


def local(
    grad_output,
    router_logits,
    expert_ids,
    router_input,
    router_weight,
    gate_weight,
    up_weight,
    down_weight,
    gate_saved,
    up_saved,
):
    expert_count, dp_count = lax.axis_size("expert"), lax.axis_size("dp")
    _, group, share = grad_output.shape
    expert_total = router_logits.shape[2]
    top = expert_ids.shape[2]
    local_experts, slots, hidden_size = gate_saved.shape
    depth = slots // expert_count
    rows = local_experts * slots
    piece = rows // dp_count
    tokens = expert_count * group
    aux = -(-(3 * expert_total + top) // LANES) * LANES
    bf16, f32 = jnp.bfloat16, jnp.float32
    paired = dp_count == local_experts and dp_count & (dp_count - 1) == 0
    cubed = paired and expert_count == 8
    sizes = (group, expert_total, top, depth)
    own_tokens = router_input.shape[1]

    def swap(value, axis, k):
        count = lax.axis_size(axis)
        return lax.ppermute(value, axis, [(j, j ^ k) for j in range(count)])

    def gather(value):
        if not cubed:
            return [lax.all_gather(value, "expert", axis=0, tiled=True)]
        parts = [value] + [swap(value, "expert", k) for k in (2, 4, 6)]
        joined = jnp.concatenate(parts, axis=0)
        return parts + [swap(joined, "expert", 1)]

    packed = call(
        functools.partial(pack_kernel, expert_total),
        ((group, aux + share), bf16),
        (router_logits, expert_ids, grad_output),
        scratch=(
            VMEM(router_logits.shape, f32),
            VMEM(expert_ids.shape, jnp.int32),
            VMEM(grad_output.shape, bf16),
            pltpu.SemaphoreType.DMA((3,)),
        ),
        flops=4 * 10**10,
        far_args=True,
    )
    token_parts = gather(packed)
    raw = [router_input] + ([swap(router_input, "expert", 1)] if cubed else [])
    sends = call(
        functools.partial(down_kernel, sizes, aux, paired, cubed, len(token_parts)),
        (((slots, hidden_size), bf16),) * local_experts,
        (*token_parts, down_weight.swapaxes(1, 2)),
    )
    if paired:
        parts = [sends[0]] + [swap(sends[k], "dp", k) for k in range(1, dp_count)]
    else:
        all_sends = jnp.concatenate(sends, axis=0).reshape(dp_count, piece, hidden_size)
        parts = list(lax.all_to_all(all_sends, "dp", 0, 0, tiled=True))
    if cubed:
        piece_shapes = (((2 * own_tokens, share), bf16),) * dp_count
    else:
        piece_shapes = (((dp_count, own_tokens, share), bf16),)
    full, slope, *pieces = call(
        functools.partial(
            table_kernel, sizes, aux, local_experts, paired, cubed, len(token_parts), len(raw)
        ),
        (((tokens, rows), f32), ((tokens, expert_total), f32), *piece_shapes),
        (*token_parts, *raw),
    )
    if cubed:
        pieces = [pieces[0]] + [swap(pieces[k], "dp", k) for k in range(1, dp_count)]
        inputs = []
    else:
        inputs = lax.all_to_all(pieces[0], "dp", 0, 0, tiled=True).reshape(group, share)
        inputs = gather(inputs)
    hidden = sum(part.astype(f32) for part in parts).astype(bf16)
    if paired:
        blocks = [hidden] + [swap(hidden, "dp", k) for k in range(1, dp_count)]
    else:
        spread = lax.all_gather(hidden, "dp", axis=0, tiled=True)
        blocks = list(spread.reshape(local_experts, slots, hidden_size))

    weights = (gate_weight, up_weight, gate_saved, up_saved)
    lanes = -(-rows // LANES) * LANES
    done = []
    for k in range(local_experts - 1):
        done += call(
            functools.partial(input_kernel, k, paired),
            (((slots, share), f32), ((1, lanes), f32)),
            (*weights, blocks[k]),
        )
    width = -(-(share + 2 * expert_count + 4 * local_experts) // LANES) * LANES
    if cubed:
        half = (expert_count // 2, group, width)
        mix_shapes = ((half, f32), (half, bf16))
    else:
        mix_shapes = (((expert_count, group, width), bf16),)
    *mixed, own = call(
        functools.partial(mix_kernel, local_experts - 1, group, paired, cubed),
        (*mix_shapes, ((tokens, LANES), f32)),
        (full, *weights, blocks[-1], *done),
        scratch=(VMEM((rows, share), f32), VMEM((1, lanes), f32)),
    )
    if cubed:
        far = swap(mixed[1], "expert", 1)
        sums = call(
            functools.partial(pair_kernel, share, expert_count, local_experts),
            (((3 * group, width), bf16),) * (expert_count // 2),
            (mixed[0], far, *pieces),
        )
        got = [sums[0]] + [swap(sums[k], "expert", 2 * k) for k in (1, 2, 3)]
    else:
        got = [lax.all_to_all(mixed[0], "expert", 0, 0, tiled=True)]
    grad_input, grad_router = call(
        functools.partial(final_kernel, sizes, paired, cubed, len(got), len(inputs), local_experts),
        (((1, group, share), bf16), ((local_experts, share), f32)),
        (*got, *inputs, own, slope, router_weight),
        scratch=(
            VMEM((1, group, share), bf16),
            VMEM((local_experts, share), f32),
            pltpu.SemaphoreType.DMA((2,)),
        ),
        far_outs=True,
    )
    return grad_input, grad_router


def solution(mesh):
    placed = (
        P("expert", None, "dp"),
        P("expert", None, None),
        P("expert", None, None),
        P("expert", "dp", None),
        P(None, "dp"),
        P("expert", "dp", None),
        P("expert", "dp", None),
        P("expert", None, "dp"),
        P("expert", None, None),
        P("expert", None, None),
    )

    return jax.shard_map(
        local,
        mesh=mesh,
        in_specs=placed,
        out_specs=(P("expert", None, "dp"), P("expert", "dp")),
        check_vma=False,
    )
```

```python
import functools

import jax
import jax.numpy as jnp
from jax import lax
from jax.experimental import pallas as pl
from jax.experimental.pallas import tpu as pltpu
from jax.sharding import PartitionSpec as P

route_scale = 2.5
LANES = 128
HIGH = lax.Precision.HIGHEST
VMEM = pltpu.VMEM
ROWS_ROWS = (((1,), (1,)), ((), ()))


def iota(shape, dim):
    return lax.broadcasted_iota(jnp.int32, shape, dim)


def place_of(block, me, paired):
    return lax.bitwise_xor(block, me) if paired else block


def call(kernel, outs, args, scratch=(), flops=0, far_args=False, far_outs=False):
    far, near = pl.BlockSpec(memory_space=pltpu.HBM), pl.BlockSpec(memory_space=VMEM)
    several = isinstance(outs[0][0], tuple)
    space = pltpu.HBM if far_outs else VMEM
    out_spec = far if far_outs else near
    arg_space = pltpu.HBM if far_args else VMEM
    return pl.pallas_call(
        kernel,
        out_shape=tuple(space(*out) for out in outs) if several else space(*outs),
        in_specs=[far if far_args else near] * len(args),
        out_specs=(out_spec,) * len(outs) if several else out_spec,
        scratch_shapes=list(scratch),
        compiler_params=pltpu.CompilerParams(vmem_limit_bytes=14 << 20),
        cost_estimate=pl.CostEstimate(flops=flops, bytes_accessed=0, transcendentals=0),
    )(*[pltpu.with_memory_space_constraint(arg, arg_space) for arg in args])


def group_of(block, count, cubed):
    if not cubed:
        return block
    doubled = 2 * block
    return lax.bitwise_xor(
        lax.rem(doubled, count) + lax.div(doubled, count), lax.axis_index("expert")
    )


def stacked(refs, stride, first, rows, columns):
    parts = []
    for ref in refs:
        for start in range(0, ref.shape[0], stride):
            parts.append(ref[start + first : start + first + rows, columns].astype(jnp.float32))
    return jnp.concatenate(parts, axis=0)


def split(values):
    upper = values.astype(jnp.bfloat16)
    return upper, (values - upper.astype(jnp.float32)).astype(jnp.bfloat16)


def chosen_piece(lines, k, paired):
    me = lax.axis_index("dp")
    found = lines[0]
    for d in range(1, len(lines)):
        found = jnp.where(place_of(k, me, paired) == d, lines[d], found)
    return found


def pack_kernel(expert_total, cubed, *refs):
    far, (out_ref, *piece_refs), held, sems = refs[:4], refs[4:-5], refs[-5:-1], refs[-1]
    fetches = [pltpu.make_async_copy(*pair, sems.at[n]) for n, pair in enumerate(zip(far, held))]
    for fetch in fetches:
        fetch.start()
    for fetch in fetches:
        fetch.wait()
    logits_ref, ids_ref, rows_ref, inputs_ref = held
    _, group, share = rows_ref.shape
    aux = out_ref.shape[1] - share
    top = ids_ref.shape[2]
    logits = logits_ref[0]
    first = logits.astype(jnp.bfloat16).astype(jnp.float32)
    rest = logits - first
    second = rest.astype(jnp.bfloat16).astype(jnp.float32)
    pieces = [first, second, rest - second, ids_ref[0].astype(jnp.float32)]
    spare = aux - 3 * expert_total - top
    if spare:
        pieces.append(jnp.zeros((group, spare), jnp.float32))
    out_ref[:group, :aux] = jnp.concatenate(pieces, axis=1).astype(jnp.bfloat16)
    out_ref[:group, aux:] = rows_ref[0]
    inputs = inputs_ref[0].astype(jnp.float32)
    lines = [inputs[:, d * share : (d + 1) * share] for d in range(inputs.shape[1] // share)]
    if cubed:
        same_ref, next_ref, across_ref = piece_refs
        found = [chosen_piece(lines, k, cubed) for k in range(4)]
        same_ref[...] = found[0].astype(jnp.bfloat16)
        next_ref[...] = jnp.concatenate([found[1], found[3]], axis=0).astype(jnp.bfloat16)
        across_ref[...] = found[2].astype(jnp.bfloat16)
    else:
        out_ref[group:, :aux] = jnp.zeros((group, aux), jnp.bfloat16)
        out_ref[group:, aux:] = jnp.concatenate(lines, axis=0).astype(jnp.bfloat16)


def routing(head, sizes, cubed):
    group, expert_total, top, depth = sizes
    tokens = head.shape[0]
    lane = iota((tokens, expert_total), 1)
    named = jnp.zeros((tokens, expert_total), jnp.float32)
    for k in range(top):
        at = 3 * expert_total + k
        named = named + (head[:, at : at + 1].astype(jnp.int32) == lane).astype(jnp.float32)
    row_at, col_at = iota((tokens, tokens), 0), iota((tokens, tokens), 1)
    earlier = (lax.div(row_at, group) == lax.div(col_at, group)) & (col_at < row_at)
    rank = jnp.dot(
        earlier.astype(jnp.bfloat16), named.astype(jnp.bfloat16), preferred_element_type=jnp.float32
    )
    block = lax.div(iota((tokens, expert_total), 0), group)
    first_slot = (group_of(block, tokens // group, cubed) * depth).astype(jnp.float32)
    return named, jnp.where(named > 0.5, first_slot + rank, -1.0)


def down_kernel(sizes, aux, paired, cubed, token_count, *refs):
    token_refs, weight_ref = refs[:token_count], refs[token_count]
    send_refs, product_ref = refs[token_count + 1 : -1], refs[-1]
    group, expert_total = sizes[:2]
    local_experts, share, _ = weight_ref.shape
    slots = send_refs[0].shape[0]
    me = lax.axis_index("dp")
    base = lax.axis_index("expert") * local_experts
    stride = group if cubed else 2 * group
    features = stacked(token_refs, stride, 0, group, slice(aux, aux + share)).astype(jnp.bfloat16)
    tokens = features.shape[0]

    def multiply(k):
        weight = weight_ref[place_of(k, me, paired)]
        product = jnp.dot(features, weight, preferred_element_type=jnp.float32)
        product_ref[k % 2] = product.astype(jnp.bfloat16)

    multiply(0)
    _, slot = routing(stacked(token_refs, stride, 0, group, slice(0, aux)), sizes, cubed)
    order = place_of(iota((8, expert_total), 0), me, paired)
    pick = (iota((8, expert_total), 1) == base + order).astype(jnp.bfloat16)
    slot_rows = lax.dot_general(
        pick, slot.astype(jnp.bfloat16), ROWS_ROWS, preferred_element_type=jnp.float32
    )
    slot_at = iota((slots, tokens), 0).astype(jnp.float32)
    for k, send_ref in enumerate(send_refs):
        if k + 1 < local_experts:
            multiply(k + 1)
        chosen = (slot_at == slot_rows[k : k + 1, :]).astype(jnp.bfloat16)
        value = jnp.dot(chosen, product_ref[k % 2], preferred_element_type=jnp.float32)
        send_ref[...] = value.astype(jnp.bfloat16)


def table_kernel(sizes, aux, local_experts, paired, cubed, token_count, *refs):
    token_refs, (*input_refs, full_ref, slope_ref, piece_ref) = refs[:token_count], refs[token_count:]
    group, expert_total = sizes[:2]
    stride = group if cubed else 2 * group
    tokens, rows = full_ref.shape
    slots = rows // local_experts
    me = lax.axis_index("dp")
    base = lax.axis_index("expert") * local_experts
    head = stacked(token_refs, stride, 0, group, slice(0, aux))
    logits = (
        head[:, :expert_total]
        + head[:, expert_total : 2 * expert_total]
        + head[:, 2 * expert_total : 3 * expert_total]
    )
    named, slot = routing(head, sizes, cubed)
    scores = jax.nn.sigmoid(logits)
    total = jnp.sum(named * scores, axis=1, keepdims=True)
    gates = route_scale * (named * scores) / total
    slope_ref[...] = named * scores * (1.0 - scores) / total
    order = place_of(lax.div(iota((expert_total, rows), 1), slots), me, paired)
    spread = (iota((expert_total, rows), 0) == base + order).astype(jnp.float32)
    slot_wide = jnp.dot(slot, spread, precision=HIGH, preferred_element_type=jnp.float32)
    gates_wide = jnp.dot(gates, spread, precision=HIGH, preferred_element_type=jnp.float32)
    wanted = lax.rem(iota((tokens, rows), 1), slots).astype(jnp.float32)
    full_ref[...] = jnp.where(slot_wide == wanted, gates_wide, 0.0)
    dp_count = lax.axis_size("dp")
    own_tokens = group // dp_count
    if cubed:
        across_ref, got_ref = input_refs
        parts = [across_ref[...].astype(jnp.float32), got_ref[own_tokens:].astype(jnp.float32)]
        piece_ref[...] = jnp.concatenate(parts, axis=0).astype(jnp.bfloat16)
        return
    features = slice(aux, token_refs[0].shape[1])
    for d in range(dp_count):
        lines = stacked(token_refs, stride, group + d * own_tokens, own_tokens, features)
        piece_ref[d] = lines.astype(jnp.bfloat16)


def expert_parts(k, paired, gate_w_ref, up_w_ref, gate_ref, up_ref, block_ref, row_ref, share_ref):
    expert = place_of(k, lax.axis_index("dp"), paired)
    hidden_grad = block_ref[...].astype(jnp.float32)
    gate_value = gate_ref[expert].astype(jnp.float32)
    up_value = up_ref[expert].astype(jnp.float32)
    sig = jax.nn.sigmoid(gate_value)
    activated = gate_value * sig
    gate_part = (hidden_grad * up_value * sig * (1.0 + gate_value * (1.0 - sig))).astype(jnp.bfloat16)
    up_part = (hidden_grad * activated).astype(jnp.bfloat16)
    value = lax.dot_general(
        gate_part, gate_w_ref[expert], ROWS_ROWS, preferred_element_type=jnp.float32
    ) + lax.dot_general(up_part, up_w_ref[expert], ROWS_ROWS, preferred_element_type=jnp.float32)
    row_ref[...] = value
    hidden = (activated * up_value).astype(jnp.bfloat16).astype(jnp.float32)
    given = jnp.sum(hidden * hidden_grad, axis=1, keepdims=True)
    slots, width = hidden_grad.shape[0], share_ref.shape[1]
    across = iota((slots, width), 0) + k * slots == iota((slots, width), 1)
    share_ref[...] = jnp.sum(jnp.where(across, given, 0.0), axis=0, keepdims=True)


def input_kernel(k, paired, *refs):
    expert_parts(k, paired, *refs)


def mix_kernel(k, group, paired, cubed, full_ref, *refs):
    weights, rest = refs[:5], refs[5:]
    if cubed:
        input_refs, rest = rest[:3], rest[3:]
    earlier, out_refs, (held_ref, share_ref) = rest[: 2 * k], rest[2 * k : -2], rest[-2:]
    slots = weights[4].shape[0]
    expert_parts(k, paired, *weights, held_ref.at[pl.ds(k * slots, slots)], share_ref)
    shares = share_ref[...]
    for at in range(k):
        held_ref[at * slots : (at + 1) * slots] = earlier[2 * at][...]
        shares = shares + earlier[2 * at + 1][...]
    full = full_ref[...]
    tokens, rows = full.shape
    local_experts = k + 1
    count = tokens // group
    share, width = held_ref.shape[1], out_refs[0].shape[2]
    given = shares[:, :rows]
    mixture = jnp.sum(full * given, axis=1, keepdims=True)
    held_lane = jnp.where(full != 0.0, given, 0.0)
    expert_at = lax.div(iota((tokens, rows), 1), slots)
    lane = iota((tokens, LANES), 1)
    own = jnp.zeros((tokens, LANES), jnp.float32)
    for e in range(local_experts):
        dg = jnp.sum(jnp.where(expert_at == e, held_lane, 0.0), axis=1, keepdims=True)
        own = own + jnp.where(lane == e, dg, 0.0)
    own_ref = out_refs[-1]
    own_ref[...] = own
    first_core = lax.rem(lax.axis_index("expert"), 2) == 0
    few = own[:, :local_experts]
    none = jnp.zeros_like(few)
    both = jnp.concatenate([jnp.where(first_core, few, none), jnp.where(first_core, none, few)], axis=1)
    row_group = group_of(lax.div(iota((tokens, count), 0), group), count, cubed)
    spread = jnp.where(row_group == iota((tokens, count), 1), mixture, 0.0)
    same = lax.rem(iota((tokens, tokens), 0), group) == lax.rem(iota((tokens, tokens), 1), group)
    same = same.astype(jnp.bfloat16)
    mix_high, mix_low = [
        jnp.dot(same, part, preferred_element_type=jnp.float32) for part in split(spread)
    ]
    own_high, own_low = [part.astype(jnp.float32) for part in split(both)]
    spare = jnp.zeros((tokens, width - share - 2 * count - 4 * local_experts), jnp.float32)
    extra = jnp.concatenate([mix_high, mix_low, own_high, own_low, spare], axis=1)
    values = held_ref[...].astype(jnp.bfloat16)
    high, low = split(full)
    mixed = jnp.dot(high, values, preferred_element_type=jnp.float32)
    mixed = mixed + jnp.dot(low, values, preferred_element_type=jnp.float32)
    at = 0
    if cubed:
        own_tokens = input_refs[0].shape[0]
        same, near, far = [ref[...].astype(jnp.float32) for ref in input_refs]
        routed = jnp.concatenate([same, near[:own_tokens], far], axis=0)
    for out_ref in out_refs[:-1]:
        blocks = out_ref.shape[0]
        if cubed:
            blocks = blocks - 1
            out_ref[blocks, :, :share] = routed.astype(out_ref.dtype)
            out_ref[blocks, :, share:] = jnp.zeros((group, width - share), out_ref.dtype)
        for q in range(blocks):
            lines = slice(at * group, (at + 1) * group)
            out_ref[q, :, :share] = mixed[lines].astype(out_ref.dtype)
            out_ref[q, :, share:] = extra[lines].astype(out_ref.dtype)
            at = at + 1


def pair_kernel(share, count, local_experts, near_ref, far_ref, *out_refs):
    group, width = near_ref.shape[1:]
    last = near_ref.shape[0] - 1
    ends = (0, count, 2 * count, 2 * count + 2 * local_experts, 2 * count + 4 * local_experts)
    for q, out_ref in enumerate(out_refs):
        total = near_ref[q] + far_ref[q].astype(jnp.float32)
        out_ref[:group, :share] = total[:, :share].astype(jnp.bfloat16)
        tail = total[:, share:]
        terms = [tail[:, i:j] for i, j in zip(ends, ends[1:])]
        sums = [terms[0] + terms[1], terms[2] + terms[3]]
        parts = [part.astype(jnp.float32) for value in sums for part in split(value)]
        parts.append(jnp.zeros((group, width - share - ends[-1]), jnp.float32))
        out_ref[:group, share:] = jnp.concatenate(parts, axis=1).astype(jnp.bfloat16)
        out_ref[group : 2 * group] = near_ref[last].astype(jnp.bfloat16)
        out_ref[2 * group :] = far_ref[last]


def ready_kernel(sizes, paired, cubed, own_ref, slope_ref, *refs):
    if cubed:
        mine_ref, slope_rows_ref, place_ref = refs
    else:
        input_refs, (mine_ref, slope_rows_ref, place_ref, inputs_ref) = refs[:-4], refs[-4:]
    group, expert_total, _, _ = sizes
    tokens = slope_ref.shape[0]
    count = tokens // group
    dp_count = lax.axis_size("dp")
    dp_me, me = lax.axis_index("dp"), lax.axis_index("expert")
    own_tokens = group // dp_count
    local_experts = expert_total // count
    row, token = iota((tokens, tokens), 1), iota((tokens, tokens), 0)
    if cubed:
        block, piece = lax.div(row, group), lax.div(lax.rem(row, group), own_tokens)
    else:
        each = count * own_tokens
        block, piece = lax.div(lax.rem(row, each), own_tokens), lax.div(row, each)
    source = block * group + place_of(piece, dp_me, paired) * own_tokens + lax.rem(row, own_tokens)
    to_row = (token == source).astype(jnp.float32)
    pick = (iota((8, LANES), 0) == iota((8, LANES), 1)).astype(jnp.float32)
    mine = lax.dot_general(
        pick, own_ref[...], ROWS_ROWS, precision=HIGH, preferred_element_type=jnp.float32
    )
    expert = me * local_experts + place_of(iota((8, expert_total), 0), dp_me, paired)
    pick = (iota((8, expert_total), 1) == expert).astype(jnp.float32)
    slopes = lax.dot_general(
        pick, slope_ref[...], ROWS_ROWS, precision=HIGH, preferred_element_type=jnp.float32
    )
    both = jnp.concatenate([route_scale * mine, slopes], axis=0)
    both = jnp.dot(both, to_row, precision=HIGH, preferred_element_type=jnp.float32)
    mine_ref[...] = both[:8]
    slope_rows_ref[...] = both[8:]
    group_at = group_of(lax.div(iota((count, tokens), 1), group), count, cubed)
    to_group = (group_at == iota((count, tokens), 0)).astype(jnp.float32)
    place_ref[:count] = jnp.dot(to_group, to_row, preferred_element_type=jnp.float32)
    in_group = lax.rem(iota((group, tokens), 1), group) == iota((group, tokens), 0)
    place_ref[count:] = jnp.dot(
        in_group.astype(jnp.float32), to_row, preferred_element_type=jnp.float32
    )
    if not cubed:
        parts = [ref[...].astype(jnp.float32) for ref in input_refs]
        inputs_ref[...] = jnp.concatenate(parts, axis=0).astype(jnp.bfloat16)


def final_kernel(sizes, paired, cubed, got_count, local_experts, *refs):
    got_refs, rest = refs[:got_count], refs[got_count:]
    mine_ref, slope_rows_ref, place_ref, *input_refs, slope_ref, weight_ref = rest[:-5]
    rest = rest[-5:]
    input_far, router_far, input_ref, router_ref, sems = rest
    group, expert_total, _, _ = sizes
    tokens = slope_ref.shape[0]
    count = tokens // group
    share = router_ref.shape[1]
    dp_me, me = lax.axis_index("dp"), lax.axis_index("expert")
    if cubed:
        sources = [(ref[:group], lax.bitwise_xor(me, 2 * b)) for b, ref in enumerate(got_refs)]
        parts = [
            ref[half * group : (half + 1) * group, :share].astype(jnp.float32)
            for half in (1, 2)
            for ref in got_refs
        ]
        inputs = jnp.concatenate(parts, axis=0).astype(jnp.bfloat16)
    else:
        sources = [(got_refs[0][j], j) for j in range(count)]
        inputs = input_refs[0][...]
    sums = jnp.zeros((group, 2 * count), jnp.float32)
    for got, _ in sources:
        sums = sums + got[:, share : share + 2 * count].astype(jnp.float32)
    mixture = sums[:, :count] + sums[:, count:]
    wide = jnp.dot(
        mixture, place_ref[:count], precision=HIGH, preferred_element_type=jnp.float32
    )
    row_mixture = jnp.sum(wide * place_ref[count:], axis=0, keepdims=True)
    lines = slope_rows_ref[...] * (mine_ref[...] - row_mixture)
    grads = jnp.dot(
        lines.astype(jnp.bfloat16), inputs, preferred_element_type=jnp.float32
    )
    for e in range(local_experts):
        place = place_of(e, dp_me, paired)
        router_ref[pl.ds(place, 1)] = grads[e : e + 1]
    last = pltpu.make_async_copy(router_ref, router_far, sems.at[1])
    last.start()
    mixed = jnp.zeros((group, share), jnp.float32)
    given = jnp.zeros((group, expert_total), jnp.float32)
    part = (4 * local_experts, expert_total)
    place = lax.rem(iota(part, 0), 2 * local_experts)
    order = place_of(lax.rem(place, local_experts), dp_me, paired)
    for got, source in sources:
        mixed = mixed + got[:, :share].astype(jnp.float32)
        first = (source - lax.rem(source, 2) + lax.div(place, local_experts)) * local_experts
        to_expert = (iota(part, 1) == first + order).astype(jnp.bfloat16)
        shares = got[:, share + 2 * count : share + 2 * count + 4 * local_experts]
        given = given + jnp.dot(shares, to_expert, preferred_element_type=jnp.float32)
    my_mixture = jnp.sum(
        jnp.where(iota((group, count), 1) == me, mixture, 0.0), axis=1, keepdims=True
    )
    if cubed:
        my_slope = slope_ref[:group, :]
    else:
        my_slope = slope_ref[pl.ds(pl.multiple_of(me * group, group), group), :]
    my_grad = (my_slope * (route_scale * given - my_mixture)).astype(jnp.bfloat16)
    routed = jnp.dot(my_grad, weight_ref[...], preferred_element_type=jnp.float32)
    input_ref[0] = (mixed + routed).astype(jnp.bfloat16)
    store = pltpu.make_async_copy(input_ref, input_far, sems.at[0])
    store.start()
    last.wait()
    store.wait()


def local(
    grad_output,
    router_logits,
    expert_ids,
    router_input,
    router_weight,
    gate_weight,
    up_weight,
    down_weight,
    gate_saved,
    up_saved,
):
    expert_count, dp_count = lax.axis_size("expert"), lax.axis_size("dp")
    _, group, share = grad_output.shape
    expert_total = router_logits.shape[2]
    top = expert_ids.shape[2]
    local_experts, slots, hidden_size = gate_saved.shape
    depth = slots // expert_count
    rows = local_experts * slots
    piece = rows // dp_count
    tokens = expert_count * group
    aux = -(-(3 * expert_total + top) // LANES) * LANES
    bf16, f32 = jnp.bfloat16, jnp.float32
    paired = dp_count == local_experts and dp_count & (dp_count - 1) == 0
    cubed = paired and dp_count == 4 and expert_count == 8
    sizes = (group, expert_total, top, depth)
    own_tokens = router_input.shape[1]

    def swap(value, axis, k):
        count = lax.axis_size(axis)
        return lax.ppermute(value, axis, [(j, j ^ k) for j in range(count)])

    def gather(value):
        if not cubed:
            return [lax.all_gather(value, "expert", axis=0, tiled=True)]
        parts = [value] + [swap(value, "expert", k) for k in (2, 4, 6)]
        joined = jnp.concatenate(parts, axis=0)
        return parts + [swap(joined, "expert", 1)]

    if cubed:
        pack_shapes = ((group, aux + share),) + tuple((n * own_tokens, share) for n in (1, 2, 1))
    else:
        pack_shapes = ((2 * group, aux + share),)
    packed, *pieces = call(
        functools.partial(pack_kernel, expert_total, cubed),
        tuple((shape, bf16) for shape in pack_shapes),
        (router_logits, expert_ids, grad_output, router_input),
        scratch=(
            VMEM(router_logits.shape, f32),
            VMEM(expert_ids.shape, jnp.int32),
            VMEM(grad_output.shape, bf16),
            VMEM(router_input.shape, bf16),
            pltpu.SemaphoreType.DMA((4,)),
        ),
        flops=4 * 10**10,
        far_args=True,
    )
    if cubed:
        pieces[1] = swap(pieces[1], "dp", 1)
    token_parts = gather(packed)
    sends = call(
        functools.partial(down_kernel, sizes, aux, paired, cubed, len(token_parts)),
        (((slots, hidden_size), bf16),) * local_experts,
        (*token_parts, down_weight.swapaxes(1, 2)),
        scratch=(VMEM((2, tokens, hidden_size), bf16),),
    )
    if paired:
        parts = [sends[0]] + [swap(sends[k], "dp", k) for k in range(1, dp_count)]
    else:
        all_sends = jnp.concatenate(sends, axis=0).reshape(dp_count, piece, hidden_size)
        parts = list(lax.all_to_all(all_sends, "dp", 0, 0, tiled=True))
    if cubed:
        piece_shape = (2 * own_tokens, share)
    else:
        piece_shape = (dp_count, expert_count * own_tokens, share)
    full, slope, piece_out = call(
        functools.partial(table_kernel, sizes, aux, local_experts, paired, cubed, len(token_parts)),
        (((tokens, rows), f32), ((tokens, expert_total), f32), (piece_shape, bf16)),
        (*token_parts, *((pieces[2], pieces[1]) if cubed else ())),
    )
    if cubed:
        pieces = [pieces[0], pieces[1], swap(piece_out, "dp", 2)]
    else:
        pieces = list(lax.all_to_all(piece_out, "dp", 0, 0, tiled=True))
    hidden = sum(part.astype(f32) for part in parts).astype(bf16)
    if paired:
        blocks = [hidden] + [swap(hidden, "dp", k) for k in range(1, dp_count)]
    else:
        spread = lax.all_gather(hidden, "dp", axis=0, tiled=True)
        blocks = list(spread.reshape(local_experts, slots, hidden_size))

    weights = (gate_weight, up_weight, gate_saved, up_saved)
    lanes = -(-rows // LANES) * LANES
    done = []
    for k in range(local_experts - 1):
        done += call(
            functools.partial(input_kernel, k, paired),
            (((slots, share), f32), ((1, lanes), f32)),
            (*weights, blocks[k]),
        )
    width = -(-(share + 2 * expert_count + 4 * local_experts) // LANES) * LANES
    if cubed:
        half = (expert_count // 2 + 1, group, width)
        mix_shapes = ((half, f32), (half, bf16))
    else:
        mix_shapes = (((expert_count, group, width), bf16),)
    *mixed, own = call(
        functools.partial(mix_kernel, local_experts - 1, group, paired, cubed),
        (*mix_shapes, ((tokens, LANES), f32)),
        (full, *weights, blocks[-1], *(pieces if cubed else ()), *done),
        scratch=(VMEM((rows, share), f32), VMEM((1, lanes), f32)),
    )
    if cubed:
        far = swap(mixed[1], "expert", 1)
        sums = call(
            functools.partial(pair_kernel, share, expert_count, local_experts),
            (((3 * group, width), bf16),) * (expert_count // 2),
            (mixed[0], far),
        )
        got = [sums[0]] + [swap(sums[k], "expert", 2 * k) for k in (1, 2, 3)]
    else:
        got = [lax.all_to_all(mixed[0], "expert", 0, 0, tiled=True)]
    ready = call(
        functools.partial(ready_kernel, sizes, paired, cubed),
        (
            ((8, tokens), f32),
            ((8, tokens), f32),
            ((expert_count + group, tokens), f32),
            *(() if cubed else (((tokens, share), bf16),)),
        ),
        (own, slope, *(() if cubed else pieces)),
    )
    grad_input, grad_router = call(
        functools.partial(final_kernel, sizes, paired, cubed, len(got), local_experts),
        (((1, group, share), bf16), ((local_experts, share), f32)),
        (*got, *ready, slope, router_weight),
        scratch=(
            VMEM((1, group, share), bf16),
            VMEM((local_experts, share), f32),
            pltpu.SemaphoreType.DMA((2,)),
        ),
        far_outs=True,
    )
    return grad_input, grad_router


def solution(mesh):
    placed = (
        P("expert", None, "dp"),
        P("expert", None, None),
        P("expert", None, None),
        P("expert", "dp", None),
        P(None, "dp"),
        P("expert", "dp", None),
        P("expert", "dp", None),
        P("expert", None, "dp"),
        P("expert", None, None),
        P("expert", None, None),
    )

    return jax.shard_map(
        local,
        mesh=mesh,
        in_specs=placed,
        out_specs=(P("expert", None, "dp"), P("expert", "dp")),
        check_vma=False,
    )
```

```python
import functools

import jax
import jax.numpy as jnp
from jax import lax
from jax.experimental import pallas as pl
from jax.experimental.pallas import tpu as pltpu
from jax.sharding import PartitionSpec as P

route_scale = 2.5
LANES = 128
HIGH = lax.Precision.HIGHEST
VMEM = pltpu.VMEM
ROWS_ROWS = (((1,), (1,)), ((), ()))


def iota(shape, dim):
    return lax.broadcasted_iota(jnp.int32, shape, dim)


def place_of(block, me, paired):
    return lax.bitwise_xor(block, me) if paired else block


def call(kernel, outs, args, scratch=(), flops=0, far_args=False, far_outs=False):
    far, near = pl.BlockSpec(memory_space=pltpu.HBM), pl.BlockSpec(memory_space=VMEM)
    several = isinstance(outs[0][0], tuple)
    space = pltpu.HBM if far_outs else VMEM
    out_spec = far if far_outs else near
    arg_space = pltpu.HBM if far_args else VMEM
    return pl.pallas_call(
        kernel,
        out_shape=tuple(space(*out) for out in outs) if several else space(*outs),
        in_specs=[far if far_args else near] * len(args),
        out_specs=(out_spec,) * len(outs) if several else out_spec,
        scratch_shapes=list(scratch),
        compiler_params=pltpu.CompilerParams(vmem_limit_bytes=14 << 20),
        cost_estimate=pl.CostEstimate(flops=flops, bytes_accessed=0, transcendentals=0),
    )(*[pltpu.with_memory_space_constraint(arg, arg_space) for arg in args])


def group_of(block, count, cubed):
    if not cubed:
        return block
    one = jnp.ones_like(block)
    row = lax.rem(block, count // 2)
    offset = lax.bitwise_xor(2 * row + lax.min(row, one), lax.div(block, count // 2))
    return lax.bitwise_xor(offset, lax.axis_index("expert"))


def stacked(refs, stride, first, rows, columns):
    parts = []
    for ref in refs:
        for start in range(0, ref.shape[0], stride):
            parts.append(ref[start + first : start + first + rows, columns].astype(jnp.float32))
    return jnp.concatenate(parts, axis=0)


def split(values):
    upper = values.astype(jnp.bfloat16)
    return upper, (values - upper.astype(jnp.float32)).astype(jnp.bfloat16)


def chosen_piece(lines, k, paired):
    me = lax.axis_index("dp")
    found = lines[0]
    for d in range(1, len(lines)):
        found = jnp.where(place_of(k, me, paired) == d, lines[d], found)
    return found


def pack_kernel(expert_total, cubed, *refs):
    far, (out_ref, *piece_refs), held, sems = refs[:4], refs[4:-5], refs[-5:-1], refs[-1]
    fetches = [pltpu.make_async_copy(*pair, sems.at[n]) for n, pair in enumerate(zip(far, held))]
    for fetch in fetches:
        fetch.start()
    for fetch in fetches:
        fetch.wait()
    logits_ref, ids_ref, rows_ref, inputs_ref = held
    _, group, share = rows_ref.shape
    aux = out_ref.shape[1] - share
    top = ids_ref.shape[2]
    logits = logits_ref[0]
    first = logits.astype(jnp.bfloat16).astype(jnp.float32)
    rest = logits - first
    second = rest.astype(jnp.bfloat16).astype(jnp.float32)
    pieces = [first, second, rest - second, ids_ref[0].astype(jnp.float32)]
    spare = aux - 3 * expert_total - top
    if spare:
        pieces.append(jnp.zeros((group, spare), jnp.float32))
    out_ref[:group, :aux] = jnp.concatenate(pieces, axis=1).astype(jnp.bfloat16)
    out_ref[:group, aux:] = rows_ref[0]
    inputs = inputs_ref[0].astype(jnp.float32)
    lines = [inputs[:, d * share : (d + 1) * share] for d in range(inputs.shape[1] // share)]
    if cubed:
        same_ref, next_ref, across_ref = piece_refs
        found = [chosen_piece(lines, k, cubed) for k in range(4)]
        same_ref[...] = found[0].astype(jnp.bfloat16)
        next_ref[...] = jnp.concatenate([found[1], found[3]], axis=0).astype(jnp.bfloat16)
        across_ref[...] = found[2].astype(jnp.bfloat16)
    else:
        out_ref[group:, :aux] = jnp.zeros((group, aux), jnp.bfloat16)
        out_ref[group:, aux:] = jnp.concatenate(lines, axis=0).astype(jnp.bfloat16)


def routing(head, sizes, cubed):
    group, expert_total, top, depth = sizes
    tokens = head.shape[0]
    lane = iota((tokens, expert_total), 1)
    named = jnp.zeros((tokens, expert_total), jnp.float32)
    for k in range(top):
        at = 3 * expert_total + k
        named = named + (head[:, at : at + 1].astype(jnp.int32) == lane).astype(jnp.float32)
    row_at, col_at = iota((tokens, tokens), 0), iota((tokens, tokens), 1)
    earlier = (lax.div(row_at, group) == lax.div(col_at, group)) & (col_at < row_at)
    rank = jnp.dot(
        earlier.astype(jnp.bfloat16), named.astype(jnp.bfloat16), preferred_element_type=jnp.float32
    )
    block = lax.div(iota((tokens, expert_total), 0), group)
    first_slot = (group_of(block, tokens // group, cubed) * depth).astype(jnp.float32)
    return named, jnp.where(named > 0.5, first_slot + rank, -1.0)


def down_kernel(sizes, aux, paired, cubed, token_count, *refs):
    token_refs, weight_ref = refs[:token_count], refs[token_count]
    send_refs, product_ref = refs[token_count + 1 : -1], refs[-1]
    group, expert_total = sizes[:2]
    local_experts, share, _ = weight_ref.shape
    slots = send_refs[0].shape[0]
    me = lax.axis_index("dp")
    base = lax.axis_index("expert") * local_experts
    stride = group if cubed else 2 * group
    features = stacked(token_refs, stride, 0, group, slice(aux, aux + share)).astype(jnp.bfloat16)
    tokens = features.shape[0]

    def multiply(k):
        weight = weight_ref[place_of(k, me, paired)]
        product = jnp.dot(features, weight, preferred_element_type=jnp.float32)
        product_ref[k % 2] = product.astype(jnp.bfloat16)

    multiply(0)
    _, slot = routing(stacked(token_refs, stride, 0, group, slice(0, aux)), sizes, cubed)
    order = place_of(iota((8, expert_total), 0), me, paired)
    pick = (iota((8, expert_total), 1) == base + order).astype(jnp.bfloat16)
    slot_rows = lax.dot_general(
        pick, slot.astype(jnp.bfloat16), ROWS_ROWS, preferred_element_type=jnp.float32
    )
    slot_at = iota((slots, tokens), 0).astype(jnp.float32)
    for k, send_ref in enumerate(send_refs):
        if k + 1 < local_experts:
            multiply(k + 1)
        chosen = (slot_at == slot_rows[k : k + 1, :]).astype(jnp.bfloat16)
        value = jnp.dot(chosen, product_ref[k % 2], preferred_element_type=jnp.float32)
        send_ref[...] = value.astype(jnp.bfloat16)


def table_kernel(sizes, aux, local_experts, paired, cubed, token_count, *refs):
    token_refs, (*input_refs, full_ref, slope_ref, piece_ref) = refs[:token_count], refs[token_count:]
    group, expert_total = sizes[:2]
    stride = group if cubed else 2 * group
    tokens, rows = full_ref.shape
    slots = rows // local_experts
    me = lax.axis_index("dp")
    base = lax.axis_index("expert") * local_experts
    head = stacked(token_refs, stride, 0, group, slice(0, aux))
    logits = (
        head[:, :expert_total]
        + head[:, expert_total : 2 * expert_total]
        + head[:, 2 * expert_total : 3 * expert_total]
    )
    named, slot = routing(head, sizes, cubed)
    scores = jax.nn.sigmoid(logits)
    total = jnp.sum(named * scores, axis=1, keepdims=True)
    gates = route_scale * (named * scores) / total
    slope_ref[...] = named * scores * (1.0 - scores) / total
    order = place_of(lax.div(iota((expert_total, rows), 1), slots), me, paired)
    spread = (iota((expert_total, rows), 0) == base + order).astype(jnp.float32)
    slot_wide = jnp.dot(slot, spread, precision=HIGH, preferred_element_type=jnp.float32)
    gates_wide = jnp.dot(gates, spread, precision=HIGH, preferred_element_type=jnp.float32)
    wanted = lax.rem(iota((tokens, rows), 1), slots).astype(jnp.float32)
    full_ref[...] = jnp.where(slot_wide == wanted, gates_wide, 0.0)
    dp_count = lax.axis_size("dp")
    own_tokens = group // dp_count
    if cubed:
        across_ref, got_ref = input_refs
        parts = [across_ref[...].astype(jnp.float32), got_ref[own_tokens:].astype(jnp.float32)]
        piece_ref[...] = jnp.concatenate(parts, axis=0).astype(jnp.bfloat16)
        return
    features = slice(aux, token_refs[0].shape[1])
    for d in range(dp_count):
        lines = stacked(token_refs, stride, group + d * own_tokens, own_tokens, features)
        piece_ref[d] = lines.astype(jnp.bfloat16)


def expert_parts(k, paired, gate_w_ref, up_w_ref, gate_ref, up_ref, block_ref, row_ref, share_ref):
    expert = place_of(k, lax.axis_index("dp"), paired)
    hidden_grad = block_ref[...].astype(jnp.float32)
    gate_value = gate_ref[expert].astype(jnp.float32)
    up_value = up_ref[expert].astype(jnp.float32)
    sig = jax.nn.sigmoid(gate_value)
    activated = gate_value * sig
    gate_part = (hidden_grad * up_value * sig * (1.0 + gate_value * (1.0 - sig))).astype(jnp.bfloat16)
    up_part = (hidden_grad * activated).astype(jnp.bfloat16)
    value = lax.dot_general(
        gate_part, gate_w_ref[expert], ROWS_ROWS, preferred_element_type=jnp.float32
    ) + lax.dot_general(up_part, up_w_ref[expert], ROWS_ROWS, preferred_element_type=jnp.float32)
    row_ref[...] = value
    hidden = (activated * up_value).astype(jnp.bfloat16).astype(jnp.float32)
    given = jnp.sum(hidden * hidden_grad, axis=1, keepdims=True)
    slots, width = hidden_grad.shape[0], share_ref.shape[1]
    across = iota((slots, width), 0) + k * slots == iota((slots, width), 1)
    share_ref[...] = jnp.sum(jnp.where(across, given, 0.0), axis=0, keepdims=True)


def input_kernel(k, paired, *refs):
    expert_parts(k, paired, *refs)


def mix_kernel(turns, group, paired, cubed, full_ref, *refs):
    k = turns[-1]
    weights, rest = refs[:5], refs[5:]
    if cubed:
        input_refs, rest = rest[:3], rest[3:]
    before = 2 * len(turns) - 2
    earlier, out_refs, (held_ref, share_ref) = rest[:before], rest[before:-2], rest[-2:]
    slots = weights[4].shape[0]
    expert_parts(k, paired, *weights, held_ref.at[pl.ds(k * slots, slots)], share_ref)
    shares = share_ref[...]
    for turn, at in enumerate(turns[:-1]):
        held_ref[at * slots : (at + 1) * slots] = earlier[2 * turn][...]
        shares = shares + earlier[2 * turn + 1][...]
    full = full_ref[...]
    tokens, rows = full.shape
    local_experts = len(turns)
    count = tokens // group
    share, width = held_ref.shape[1], out_refs[0].shape[2]
    given = shares[:, :rows]
    mixture = jnp.sum(full * given, axis=1, keepdims=True)
    held_lane = jnp.where(full != 0.0, given, 0.0)
    expert_at = lax.div(iota((tokens, rows), 1), slots)
    lane = iota((tokens, LANES), 1)
    own = jnp.zeros((tokens, LANES), jnp.float32)
    for e in range(local_experts):
        dg = jnp.sum(jnp.where(expert_at == e, held_lane, 0.0), axis=1, keepdims=True)
        own = own + jnp.where(lane == e, dg, 0.0)
    own_ref = out_refs[-1]
    own_ref[...] = own
    first_core = lax.rem(lax.axis_index("expert"), 2) == 0
    few = own[:, :local_experts]
    none = jnp.zeros_like(few)
    both = jnp.concatenate([jnp.where(first_core, few, none), jnp.where(first_core, none, few)], axis=1)
    row_group = group_of(lax.div(iota((tokens, count), 0), group), count, cubed)
    spread = jnp.where(row_group == iota((tokens, count), 1), mixture, 0.0)
    same = lax.rem(iota((tokens, tokens), 0), group) == lax.rem(iota((tokens, tokens), 1), group)
    same = same.astype(jnp.bfloat16)
    mix_high, mix_low = [
        jnp.dot(same, part, preferred_element_type=jnp.float32) for part in split(spread)
    ]
    own_high, own_low = [part.astype(jnp.float32) for part in split(both)]
    spare = jnp.zeros((tokens, width - share - 2 * count - 4 * local_experts), jnp.float32)
    extra = jnp.concatenate([mix_high, mix_low, own_high, own_low, spare], axis=1)
    values = held_ref[...].astype(jnp.bfloat16)
    high, low = split(full)
    mixed = jnp.dot(high, values, preferred_element_type=jnp.float32)
    mixed = mixed + jnp.dot(low, values, preferred_element_type=jnp.float32)
    at = 0
    if cubed:
        own_tokens = input_refs[0].shape[0]
        same, near, far = [ref[...].astype(jnp.float32) for ref in input_refs]
        routed = jnp.concatenate([same, near[:own_tokens], far], axis=0)
    for out_ref in out_refs[:-1]:
        blocks = out_ref.shape[0]
        if cubed:
            blocks = blocks - 1
            out_ref[blocks, :, :share] = routed.astype(out_ref.dtype)
            out_ref[blocks, :, share:] = jnp.zeros((group, width - share), out_ref.dtype)
        for q in range(blocks):
            block = at
            if cubed and at % (count // 2):
                block = (at + count // 2) % count
            lines = slice(block * group, (block + 1) * group)
            out_ref[q, :, :share] = mixed[lines].astype(out_ref.dtype)
            out_ref[q, :, share:] = extra[lines].astype(out_ref.dtype)
            at = at + 1


def pair_kernel(share, count, local_experts, near_ref, far_ref, *out_refs):
    group, width = near_ref.shape[1:]
    last = near_ref.shape[0] - 1
    ends = (0, count, 2 * count, 2 * count + 2 * local_experts, 2 * count + 4 * local_experts)
    for q, out_ref in enumerate(out_refs):
        total = near_ref[q] + far_ref[q].astype(jnp.float32)
        out_ref[:group, :share] = total[:, :share].astype(jnp.bfloat16)
        tail = total[:, share:]
        terms = [tail[:, i:j] for i, j in zip(ends, ends[1:])]
        sums = [terms[0] + terms[1], terms[2] + terms[3]]
        parts = [part.astype(jnp.float32) for value in sums for part in split(value)]
        parts.append(jnp.zeros((group, width - share - ends[-1]), jnp.float32))
        out_ref[:group, share:] = jnp.concatenate(parts, axis=1).astype(jnp.bfloat16)
        out_ref[group : 2 * group] = near_ref[last].astype(jnp.bfloat16)
        out_ref[2 * group :] = far_ref[last]


def ready_kernel(sizes, paired, cubed, own_ref, slope_ref, *refs):
    if cubed:
        mine_ref, slope_rows_ref, place_ref = refs
    else:
        input_refs, (mine_ref, slope_rows_ref, place_ref, inputs_ref) = refs[:-4], refs[-4:]
    group, expert_total, _, _ = sizes
    tokens = slope_ref.shape[0]
    count = tokens // group
    dp_count = lax.axis_size("dp")
    dp_me, me = lax.axis_index("dp"), lax.axis_index("expert")
    own_tokens = group // dp_count
    local_experts = expert_total // count
    row, token = iota((tokens, tokens), 1), iota((tokens, tokens), 0)
    if cubed:
        place, piece = lax.div(row, group), lax.div(lax.rem(row, group), own_tokens)
        other = lax.rem(place + count // 2, count)
        block = jnp.where(lax.rem(place, count // 2) == 0, place, other)
    else:
        each = count * own_tokens
        block, piece = lax.div(lax.rem(row, each), own_tokens), lax.div(row, each)
    source = block * group + place_of(piece, dp_me, paired) * own_tokens + lax.rem(row, own_tokens)
    to_row = (token == source).astype(jnp.float32)
    pick = (iota((8, LANES), 0) == iota((8, LANES), 1)).astype(jnp.float32)
    mine = lax.dot_general(
        pick, own_ref[...], ROWS_ROWS, precision=HIGH, preferred_element_type=jnp.float32
    )
    expert = me * local_experts + place_of(iota((8, expert_total), 0), dp_me, paired)
    pick = (iota((8, expert_total), 1) == expert).astype(jnp.float32)
    slopes = lax.dot_general(
        pick, slope_ref[...], ROWS_ROWS, precision=HIGH, preferred_element_type=jnp.float32
    )
    both = jnp.concatenate([route_scale * mine, slopes], axis=0)
    both = jnp.dot(both, to_row, precision=HIGH, preferred_element_type=jnp.float32)
    mine_ref[...] = both[:8]
    slope_rows_ref[...] = both[8:]
    group_at = group_of(lax.div(iota((count, tokens), 1), group), count, cubed)
    to_group = (group_at == iota((count, tokens), 0)).astype(jnp.float32)
    place_ref[:count] = jnp.dot(to_group, to_row, preferred_element_type=jnp.float32)
    in_group = lax.rem(iota((group, tokens), 1), group) == iota((group, tokens), 0)
    place_ref[count:] = jnp.dot(
        in_group.astype(jnp.float32), to_row, preferred_element_type=jnp.float32
    )
    if not cubed:
        parts = [ref[...].astype(jnp.float32) for ref in input_refs]
        inputs_ref[...] = jnp.concatenate(parts, axis=0).astype(jnp.bfloat16)


def final_kernel(sizes, paired, cubed, got_count, local_experts, *refs):
    got_refs, rest = refs[:got_count], refs[got_count:]
    mine_ref, slope_rows_ref, place_ref, *input_refs, slope_ref, weight_ref = rest[:-5]
    rest = rest[-5:]
    input_far, router_far, input_ref, router_ref, sems = rest
    group, expert_total, _, _ = sizes
    tokens = slope_ref.shape[0]
    count = tokens // group
    share = router_ref.shape[1]
    dp_me, me = lax.axis_index("dp"), lax.axis_index("expert")
    if cubed:
        sources = [(ref[:group], lax.bitwise_xor(me, 2 * b)) for b, ref in enumerate(got_refs)]
        parts = [
            ref[half * group : (half + 1) * group, :share].astype(jnp.float32)
            for half in (1, 2)
            for ref in got_refs
        ]
        inputs = jnp.concatenate(parts, axis=0).astype(jnp.bfloat16)
    else:
        sources = [(got_refs[0][j], j) for j in range(count)]
        inputs = input_refs[0][...]
    sums = jnp.zeros((group, 2 * count), jnp.float32)
    for got, _ in sources:
        sums = sums + got[:, share : share + 2 * count].astype(jnp.float32)
    mixture = sums[:, :count] + sums[:, count:]
    wide = jnp.dot(
        mixture, place_ref[:count], precision=HIGH, preferred_element_type=jnp.float32
    )
    row_mixture = jnp.sum(wide * place_ref[count:], axis=0, keepdims=True)
    lines = slope_rows_ref[...] * (mine_ref[...] - row_mixture)
    grads = jnp.dot(
        lines.astype(jnp.bfloat16), inputs, preferred_element_type=jnp.float32
    )
    for e in range(local_experts):
        place = place_of(e, dp_me, paired)
        router_ref[pl.ds(place, 1)] = grads[e : e + 1]
    last = pltpu.make_async_copy(router_ref, router_far, sems.at[1])
    last.start()
    mixed = jnp.zeros((group, share), jnp.float32)
    given = jnp.zeros((group, expert_total), jnp.float32)
    part = (4 * local_experts, expert_total)
    place = lax.rem(iota(part, 0), 2 * local_experts)
    order = place_of(lax.rem(place, local_experts), dp_me, paired)
    for got, source in sources:
        mixed = mixed + got[:, :share].astype(jnp.float32)
        first = (source - lax.rem(source, 2) + lax.div(place, local_experts)) * local_experts
        to_expert = (iota(part, 1) == first + order).astype(jnp.bfloat16)
        shares = got[:, share + 2 * count : share + 2 * count + 4 * local_experts]
        given = given + jnp.dot(shares, to_expert, preferred_element_type=jnp.float32)
    my_mixture = jnp.sum(
        jnp.where(iota((group, count), 1) == me, mixture, 0.0), axis=1, keepdims=True
    )
    if cubed:
        my_slope = slope_ref[:group, :]
    else:
        my_slope = slope_ref[pl.ds(pl.multiple_of(me * group, group), group), :]
    my_grad = (my_slope * (route_scale * given - my_mixture)).astype(jnp.bfloat16)
    routed = jnp.dot(my_grad, weight_ref[...], preferred_element_type=jnp.float32)
    input_ref[0] = (mixed + routed).astype(jnp.bfloat16)
    store = pltpu.make_async_copy(input_ref, input_far, sems.at[0])
    store.start()
    last.wait()
    store.wait()


def local(
    grad_output,
    router_logits,
    expert_ids,
    router_input,
    router_weight,
    gate_weight,
    up_weight,
    down_weight,
    gate_saved,
    up_saved,
):
    expert_count, dp_count = lax.axis_size("expert"), lax.axis_size("dp")
    _, group, share = grad_output.shape
    expert_total = router_logits.shape[2]
    top = expert_ids.shape[2]
    local_experts, slots, hidden_size = gate_saved.shape
    depth = slots // expert_count
    rows = local_experts * slots
    piece = rows // dp_count
    tokens = expert_count * group
    aux = -(-(3 * expert_total + top) // LANES) * LANES
    bf16, f32 = jnp.bfloat16, jnp.float32
    paired = dp_count == local_experts and dp_count & (dp_count - 1) == 0
    cubed = paired and dp_count == 4 and expert_count == 8
    sizes = (group, expert_total, top, depth)
    own_tokens = router_input.shape[1]

    def swap(value, axis, k):
        count = lax.axis_size(axis)
        return lax.ppermute(value, axis, [(j, j ^ k) for j in range(count)])

    def cross(value, k):
        there = [(d ^ k) * expert_count + (e ^ 1) for d in range(dp_count) for e in range(expert_count)]
        return lax.ppermute(value, ("dp", "expert"), list(enumerate(there)))

    def gather(value):
        if not cubed:
            return [lax.all_gather(value, "expert", axis=0, tiled=True)]
        parts = [value] + [swap(value, "expert", k) for k in (3, 5, 7)]
        joined = jnp.concatenate(parts, axis=0)
        return parts + [swap(joined, "expert", 1)]

    if cubed:
        pack_shapes = ((group, aux + share),) + tuple((n * own_tokens, share) for n in (1, 2, 1))
    else:
        pack_shapes = ((2 * group, aux + share),)
    packed, *pieces = call(
        functools.partial(pack_kernel, expert_total, cubed),
        tuple((shape, bf16) for shape in pack_shapes),
        (router_logits, expert_ids, grad_output, router_input),
        scratch=(
            VMEM(router_logits.shape, f32),
            VMEM(expert_ids.shape, jnp.int32),
            VMEM(grad_output.shape, bf16),
            VMEM(router_input.shape, bf16),
            pltpu.SemaphoreType.DMA((4,)),
        ),
        flops=4 * 10**10,
        far_args=True,
    )
    if cubed:
        pieces[1] = swap(pieces[1], "dp", 1)
    token_parts = gather(packed)
    sends = call(
        functools.partial(down_kernel, sizes, aux, paired, cubed, len(token_parts)),
        (((slots, hidden_size), bf16),) * local_experts,
        (*token_parts, down_weight.swapaxes(1, 2)),
        scratch=(VMEM((2, tokens, hidden_size), bf16),),
    )
    if cubed:
        parts = [cross(sends[k], k) for k in range(dp_count)]
    elif paired:
        parts = [sends[0]] + [swap(sends[k], "dp", k) for k in range(1, dp_count)]
    else:
        all_sends = jnp.concatenate(sends, axis=0).reshape(dp_count, piece, hidden_size)
        parts = list(lax.all_to_all(all_sends, "dp", 0, 0, tiled=True))
    if cubed:
        piece_shape = (2 * own_tokens, share)
    else:
        piece_shape = (dp_count, expert_count * own_tokens, share)
    full, slope, piece_out = call(
        functools.partial(table_kernel, sizes, aux, local_experts, paired, cubed, len(token_parts)),
        (((tokens, rows), f32), ((tokens, expert_total), f32), (piece_shape, bf16)),
        (*token_parts, *((pieces[2], pieces[1]) if cubed else ())),
    )
    if cubed:
        pieces = [pieces[0], pieces[1], swap(piece_out, "dp", 2)]
    else:
        pieces = list(lax.all_to_all(piece_out, "dp", 0, 0, tiled=True))
    hidden = sum(part.astype(f32) for part in parts).astype(bf16)
    if cubed:
        blocks = [cross(hidden, k) for k in range(dp_count)]
    elif paired:
        blocks = [hidden] + [swap(hidden, "dp", k) for k in range(1, dp_count)]
    else:
        spread = lax.all_gather(hidden, "dp", axis=0, tiled=True)
        blocks = list(spread.reshape(local_experts, slots, hidden_size))

    weights = (gate_weight, up_weight, gate_saved, up_saved)
    lanes = -(-rows // LANES) * LANES
    done = []
    turns = (0, 2, 3, 1) if cubed else tuple(range(local_experts))
    for k in turns[:-1]:
        done += call(
            functools.partial(input_kernel, k, paired),
            (((slots, share), f32), ((1, lanes), f32)),
            (*weights, blocks[k]),
        )
    width = -(-(share + 2 * expert_count + 4 * local_experts) // LANES) * LANES
    if cubed:
        half = (expert_count // 2 + 1, group, width)
        mix_shapes = ((half, f32), (half, bf16))
    else:
        mix_shapes = (((expert_count, group, width), bf16),)
    *mixed, own = call(
        functools.partial(mix_kernel, turns, group, paired, cubed),
        (*mix_shapes, ((tokens, LANES), f32)),
        (full, *weights, blocks[turns[-1]], *(pieces if cubed else ()), *done),
        scratch=(VMEM((rows, share), f32), VMEM((1, lanes), f32)),
    )
    if cubed:
        far = swap(mixed[1], "expert", 1)
        sums = call(
            functools.partial(pair_kernel, share, expert_count, local_experts),
            (((3 * group, width), bf16),) * (expert_count // 2),
            (mixed[0], far),
        )
        got = [sums[0]] + [swap(sums[k], "expert", 2 * k) for k in (1, 2, 3)]
    else:
        got = [lax.all_to_all(mixed[0], "expert", 0, 0, tiled=True)]
    ready = call(
        functools.partial(ready_kernel, sizes, paired, cubed),
        (
            ((8, tokens), f32),
            ((8, tokens), f32),
            ((expert_count + group, tokens), f32),
            *(() if cubed else (((tokens, share), bf16),)),
        ),
        (own, slope, *(() if cubed else pieces)),
    )
    grad_input, grad_router = call(
        functools.partial(final_kernel, sizes, paired, cubed, len(got), local_experts),
        (((1, group, share), bf16), ((local_experts, share), f32)),
        (*got, *ready, slope, router_weight),
        scratch=(
            VMEM((1, group, share), bf16),
            VMEM((local_experts, share), f32),
            pltpu.SemaphoreType.DMA((2,)),
        ),
        far_outs=True,
    )
    return grad_input, grad_router


def solution(mesh):
    placed = (
        P("expert", None, "dp"),
        P("expert", None, None),
        P("expert", None, None),
        P("expert", "dp", None),
        P(None, "dp"),
        P("expert", "dp", None),
        P("expert", "dp", None),
        P("expert", None, "dp"),
        P("expert", None, None),
        P("expert", None, None),
    )

    return jax.shard_map(
        local,
        mesh=mesh,
        in_specs=placed,
        out_specs=(P("expert", None, "dp"), P("expert", "dp")),
        check_vma=False,
    )
```

```python
import functools

import jax
import jax.numpy as jnp
from jax import lax
from jax.experimental import pallas as pl
from jax.experimental.pallas import tpu as pltpu
from jax.sharding import PartitionSpec as P

route_scale = 2.5
LANES = 128
HIGH = lax.Precision.HIGHEST
VMEM = pltpu.VMEM
ROWS_ROWS = (((1,), (1,)), ((), ()))


def iota(shape, dim):
    return lax.broadcasted_iota(jnp.int32, shape, dim)


def place_of(block, me, paired):
    return lax.bitwise_xor(block, me) if paired else block


def call(kernel, outs, args, scratch=(), flops=0, far_args=False, far_outs=False):
    far, near = pl.BlockSpec(memory_space=pltpu.HBM), pl.BlockSpec(memory_space=VMEM)
    several = isinstance(outs[0][0], tuple)
    space = pltpu.HBM if far_outs else VMEM
    out_spec = far if far_outs else near
    arg_space = pltpu.HBM if far_args else VMEM
    return pl.pallas_call(
        kernel,
        out_shape=tuple(space(*out) for out in outs) if several else space(*outs),
        in_specs=[far if far_args else near] * len(args),
        out_specs=(out_spec,) * len(outs) if several else out_spec,
        scratch_shapes=list(scratch),
        compiler_params=pltpu.CompilerParams(vmem_limit_bytes=14 << 20),
        cost_estimate=pl.CostEstimate(flops=flops, bytes_accessed=0, transcendentals=0),
    )(*[pltpu.with_memory_space_constraint(arg, arg_space) for arg in args])


def group_of(block, count, cubed):
    if not cubed:
        return block
    one = jnp.ones_like(block)
    row = lax.rem(block, count // 2)
    offset = lax.bitwise_xor(2 * row + lax.min(row, one), lax.div(block, count // 2))
    return lax.bitwise_xor(offset, lax.axis_index("expert"))


def stacked(refs, stride, first, rows, columns):
    parts = []
    for ref in refs:
        for start in range(0, ref.shape[0], stride):
            parts.append(ref[start + first : start + first + rows, columns].astype(jnp.float32))
    return jnp.concatenate(parts, axis=0)


def split(values):
    upper = values.astype(jnp.bfloat16)
    return upper, (values - upper.astype(jnp.float32)).astype(jnp.bfloat16)


def chosen_piece(lines, k, paired):
    me = lax.axis_index("dp")
    found = lines[0]
    for d in range(1, len(lines)):
        found = jnp.where(place_of(k, me, paired) == d, lines[d], found)
    return found


def pack_kernel(expert_total, cubed, *refs):
    far, (out_ref, *piece_refs), held, sems = refs[:4], refs[4:-5], refs[-5:-1], refs[-1]
    fetches = [pltpu.make_async_copy(*pair, sems.at[n]) for n, pair in enumerate(zip(far, held))]
    for fetch in fetches:
        fetch.start()
    for fetch in fetches:
        fetch.wait()
    logits_ref, ids_ref, rows_ref, inputs_ref = held
    _, group, share = rows_ref.shape
    aux = out_ref.shape[1] - share
    top = ids_ref.shape[2]
    logits = logits_ref[0]
    first = logits.astype(jnp.bfloat16).astype(jnp.float32)
    rest = logits - first
    second = rest.astype(jnp.bfloat16).astype(jnp.float32)
    pieces = [first, second, rest - second, ids_ref[0].astype(jnp.float32)]
    spare = aux - 3 * expert_total - top
    if spare:
        pieces.append(jnp.zeros((group, spare), jnp.float32))
    out_ref[:group, :aux] = jnp.concatenate(pieces, axis=1).astype(jnp.bfloat16)
    out_ref[:group, aux:] = rows_ref[0]
    inputs = inputs_ref[0].astype(jnp.float32)
    lines = [inputs[:, d * share : (d + 1) * share] for d in range(inputs.shape[1] // share)]
    if cubed:
        same_ref, next_ref, across_ref = piece_refs
        found = [chosen_piece(lines, k, cubed) for k in range(4)]
        same_ref[...] = found[0].astype(jnp.bfloat16)
        next_ref[...] = jnp.concatenate([found[1], found[3]], axis=0).astype(jnp.bfloat16)
        across_ref[...] = found[2].astype(jnp.bfloat16)
    else:
        out_ref[group:, :aux] = jnp.zeros((group, aux), jnp.bfloat16)
        out_ref[group:, aux:] = jnp.concatenate(lines, axis=0).astype(jnp.bfloat16)


def keep_kernel(value_ref, out_ref):
    out_ref[...] = value_ref[...]


def routing(head, sizes, cubed):
    group, expert_total, top, depth = sizes
    tokens = head.shape[0]
    lane = iota((tokens, expert_total), 1)
    named = jnp.zeros((tokens, expert_total), jnp.float32)
    for k in range(top):
        at = 3 * expert_total + k
        named = named + (head[:, at : at + 1].astype(jnp.int32) == lane).astype(jnp.float32)
    row_at, col_at = iota((tokens, tokens), 0), iota((tokens, tokens), 1)
    earlier = (lax.div(row_at, group) == lax.div(col_at, group)) & (col_at < row_at)
    rank = jnp.dot(
        earlier.astype(jnp.bfloat16), named.astype(jnp.bfloat16), preferred_element_type=jnp.float32
    )
    block = lax.div(iota((tokens, expert_total), 0), group)
    first_slot = (group_of(block, tokens // group, cubed) * depth).astype(jnp.float32)
    return named, jnp.where(named > 0.5, first_slot + rank, -1.0)


def down_kernel(sizes, aux, paired, cubed, token_count, *refs):
    token_refs, weight_ref = refs[:token_count], refs[token_count]
    send_refs, product_ref = refs[token_count + 1 : -1], refs[-1]
    group, expert_total = sizes[:2]
    local_experts, share, _ = weight_ref.shape
    slots = send_refs[0].shape[0]
    me = lax.axis_index("dp")
    base = lax.axis_index("expert") * local_experts
    stride = group if cubed else 2 * group
    features = stacked(token_refs, stride, 0, group, slice(aux, aux + share)).astype(jnp.bfloat16)
    tokens = features.shape[0]

    def multiply(k):
        weight = weight_ref[place_of(k, me, paired)]
        product = jnp.dot(features, weight, preferred_element_type=jnp.float32)
        product_ref[k % 2] = product.astype(jnp.bfloat16)

    multiply(0)
    _, slot = routing(stacked(token_refs, stride, 0, group, slice(0, aux)), sizes, cubed)
    order = place_of(iota((8, expert_total), 0), me, paired)
    pick = (iota((8, expert_total), 1) == base + order).astype(jnp.bfloat16)
    slot_rows = lax.dot_general(
        pick, slot.astype(jnp.bfloat16), ROWS_ROWS, preferred_element_type=jnp.float32
    )
    slot_at = iota((slots, tokens), 0).astype(jnp.float32)
    for k, send_ref in enumerate(send_refs):
        if k + 1 < local_experts:
            multiply(k + 1)
        chosen = (slot_at == slot_rows[k : k + 1, :]).astype(jnp.bfloat16)
        value = jnp.dot(chosen, product_ref[k % 2], preferred_element_type=jnp.float32)
        send_ref[...] = value.astype(jnp.bfloat16)


def table_kernel(sizes, aux, local_experts, paired, cubed, token_count, *refs):
    token_refs, (*input_refs, full_ref, slope_ref, piece_ref) = refs[:token_count], refs[token_count:]
    group, expert_total = sizes[:2]
    stride = group if cubed else 2 * group
    tokens, rows = full_ref.shape
    slots = rows // local_experts
    me = lax.axis_index("dp")
    base = lax.axis_index("expert") * local_experts
    head = stacked(token_refs, stride, 0, group, slice(0, aux))
    logits = (
        head[:, :expert_total]
        + head[:, expert_total : 2 * expert_total]
        + head[:, 2 * expert_total : 3 * expert_total]
    )
    named, slot = routing(head, sizes, cubed)
    scores = jax.nn.sigmoid(logits)
    total = jnp.sum(named * scores, axis=1, keepdims=True)
    gates = route_scale * (named * scores) / total
    slope_ref[...] = named * scores * (1.0 - scores) / total
    order = place_of(lax.div(iota((expert_total, rows), 1), slots), me, paired)
    spread = (iota((expert_total, rows), 0) == base + order).astype(jnp.float32)
    slot_wide = jnp.dot(slot, spread, precision=HIGH, preferred_element_type=jnp.float32)
    gates_wide = jnp.dot(gates, spread, precision=HIGH, preferred_element_type=jnp.float32)
    wanted = lax.rem(iota((tokens, rows), 1), slots).astype(jnp.float32)
    full_ref[...] = jnp.where(slot_wide == wanted, gates_wide, 0.0)
    dp_count = lax.axis_size("dp")
    own_tokens = group // dp_count
    if cubed:
        across_ref, got_ref = input_refs
        parts = [across_ref[...].astype(jnp.float32), got_ref[own_tokens:].astype(jnp.float32)]
        piece_ref[...] = jnp.concatenate(parts, axis=0).astype(jnp.bfloat16)
        return
    features = slice(aux, token_refs[0].shape[1])
    for d in range(dp_count):
        lines = stacked(token_refs, stride, group + d * own_tokens, own_tokens, features)
        piece_ref[d] = lines.astype(jnp.bfloat16)


def expert_parts(k, paired, gate_w_ref, up_w_ref, gate_ref, up_ref, block_ref, row_ref, share_ref):
    expert = place_of(k, lax.axis_index("dp"), paired)
    hidden_grad = block_ref[...].astype(jnp.float32)
    gate_value = gate_ref[expert].astype(jnp.float32)
    up_value = up_ref[expert].astype(jnp.float32)
    sig = jax.nn.sigmoid(gate_value)
    activated = gate_value * sig
    gate_part = (hidden_grad * up_value * sig * (1.0 + gate_value * (1.0 - sig))).astype(jnp.bfloat16)
    up_part = (hidden_grad * activated).astype(jnp.bfloat16)
    value = lax.dot_general(
        gate_part, gate_w_ref[expert], ROWS_ROWS, preferred_element_type=jnp.float32
    ) + lax.dot_general(up_part, up_w_ref[expert], ROWS_ROWS, preferred_element_type=jnp.float32)
    row_ref[...] = value
    hidden = (activated * up_value).astype(jnp.bfloat16).astype(jnp.float32)
    given = jnp.sum(hidden * hidden_grad, axis=1, keepdims=True)
    slots, width = hidden_grad.shape[0], share_ref.shape[1]
    across = iota((slots, width), 0) + k * slots == iota((slots, width), 1)
    share_ref[...] = jnp.sum(jnp.where(across, given, 0.0), axis=0, keepdims=True)


def input_kernel(k, paired, *refs):
    expert_parts(k, paired, *refs)


def mix_kernel(turns, group, paired, cubed, full_ref, *refs):
    k = turns[-1]
    weights, rest = refs[:5], refs[5:]
    if cubed:
        input_refs, rest = rest[:3], rest[3:]
    before = 2 * len(turns) - 2
    earlier, out_refs, (held_ref, share_ref) = rest[:before], rest[before:-2], rest[-2:]
    slots = weights[4].shape[0]
    expert_parts(k, paired, *weights, held_ref.at[pl.ds(k * slots, slots)], share_ref)
    shares = share_ref[...]
    for turn, at in enumerate(turns[:-1]):
        held_ref[at * slots : (at + 1) * slots] = earlier[2 * turn][...]
        shares = shares + earlier[2 * turn + 1][...]
    full = full_ref[...]
    tokens, rows = full.shape
    local_experts = len(turns)
    count = tokens // group
    share, width = held_ref.shape[1], out_refs[0].shape[2]
    given = shares[:, :rows]
    mixture = jnp.sum(full * given, axis=1, keepdims=True)
    held_lane = jnp.where(full != 0.0, given, 0.0)
    expert_at = lax.div(iota((tokens, rows), 1), slots)
    lane = iota((tokens, LANES), 1)
    own = jnp.zeros((tokens, LANES), jnp.float32)
    for e in range(local_experts):
        dg = jnp.sum(jnp.where(expert_at == e, held_lane, 0.0), axis=1, keepdims=True)
        own = own + jnp.where(lane == e, dg, 0.0)
    own_ref = out_refs[-1]
    own_ref[...] = own
    first_core = lax.rem(lax.axis_index("expert"), 2) == 0
    few = own[:, :local_experts]
    none = jnp.zeros_like(few)
    both = jnp.concatenate([jnp.where(first_core, few, none), jnp.where(first_core, none, few)], axis=1)
    row_group = group_of(lax.div(iota((tokens, count), 0), group), count, cubed)
    spread = jnp.where(row_group == iota((tokens, count), 1), mixture, 0.0)
    same = lax.rem(iota((tokens, tokens), 0), group) == lax.rem(iota((tokens, tokens), 1), group)
    same = same.astype(jnp.bfloat16)
    mix_high, mix_low = [
        jnp.dot(same, part, preferred_element_type=jnp.float32) for part in split(spread)
    ]
    own_high, own_low = [part.astype(jnp.float32) for part in split(both)]
    spare = jnp.zeros((tokens, width - share - 2 * count - 4 * local_experts), jnp.float32)
    extra = jnp.concatenate([mix_high, mix_low, own_high, own_low, spare], axis=1)
    values = held_ref[...].astype(jnp.bfloat16)
    high, low = split(full)
    mixed = jnp.dot(high, values, preferred_element_type=jnp.float32)
    mixed = mixed + jnp.dot(low, values, preferred_element_type=jnp.float32)
    at = 0
    if cubed:
        own_tokens = input_refs[0].shape[0]
        same, near, far = [ref[...].astype(jnp.float32) for ref in input_refs]
        routed = jnp.concatenate([same, near[:own_tokens], far], axis=0)
    for out_ref in out_refs[:-1]:
        blocks = out_ref.shape[0]
        if cubed:
            blocks = blocks - 1
            out_ref[blocks, :, :share] = routed.astype(out_ref.dtype)
            out_ref[blocks, :, share:] = jnp.zeros((group, width - share), out_ref.dtype)
        for q in range(blocks):
            block = at
            if cubed and at % (count // 2):
                block = (at + count // 2) % count
            lines = slice(block * group, (block + 1) * group)
            out_ref[q, :, :share] = mixed[lines].astype(out_ref.dtype)
            out_ref[q, :, share:] = extra[lines].astype(out_ref.dtype)
            at = at + 1


def pair_kernel(share, count, local_experts, near_ref, far_ref, *out_refs):
    group, width = near_ref.shape[1:]
    last = near_ref.shape[0] - 1
    ends = (0, count, 2 * count, 2 * count + 2 * local_experts, 2 * count + 4 * local_experts)
    for q, out_ref in enumerate(out_refs):
        total = near_ref[q] + far_ref[q].astype(jnp.float32)
        out_ref[:group, :share] = total[:, :share].astype(jnp.bfloat16)
        tail = total[:, share:]
        terms = [tail[:, i:j] for i, j in zip(ends, ends[1:])]
        sums = [terms[0] + terms[1], terms[2] + terms[3]]
        parts = [part.astype(jnp.float32) for value in sums for part in split(value)]
        parts.append(jnp.zeros((group, width - share - ends[-1]), jnp.float32))
        out_ref[:group, share:] = jnp.concatenate(parts, axis=1).astype(jnp.bfloat16)
        out_ref[group : 2 * group] = near_ref[last].astype(jnp.bfloat16)
        out_ref[2 * group :] = far_ref[last]


def ready_kernel(sizes, paired, cubed, own_ref, slope_ref, *refs):
    if cubed:
        mine_ref, slope_rows_ref, place_ref = refs
    else:
        input_refs, (mine_ref, slope_rows_ref, place_ref, inputs_ref) = refs[:-4], refs[-4:]
    group, expert_total, _, _ = sizes
    tokens = slope_ref.shape[0]
    count = tokens // group
    dp_count = lax.axis_size("dp")
    dp_me, me = lax.axis_index("dp"), lax.axis_index("expert")
    own_tokens = group // dp_count
    local_experts = expert_total // count
    row, token = iota((tokens, tokens), 1), iota((tokens, tokens), 0)
    if cubed:
        place, piece = lax.div(row, group), lax.div(lax.rem(row, group), own_tokens)
        other = lax.rem(place + count // 2, count)
        block = jnp.where(lax.rem(place, count // 2) == 0, place, other)
    else:
        each = count * own_tokens
        block, piece = lax.div(lax.rem(row, each), own_tokens), lax.div(row, each)
    source = block * group + place_of(piece, dp_me, paired) * own_tokens + lax.rem(row, own_tokens)
    to_row = (token == source).astype(jnp.float32)
    pick = (iota((8, LANES), 0) == iota((8, LANES), 1)).astype(jnp.float32)
    mine = lax.dot_general(
        pick, own_ref[...], ROWS_ROWS, precision=HIGH, preferred_element_type=jnp.float32
    )
    expert = me * local_experts + place_of(iota((8, expert_total), 0), dp_me, paired)
    pick = (iota((8, expert_total), 1) == expert).astype(jnp.float32)
    slopes = lax.dot_general(
        pick, slope_ref[...], ROWS_ROWS, precision=HIGH, preferred_element_type=jnp.float32
    )
    both = jnp.concatenate([route_scale * mine, slopes], axis=0)
    both = jnp.dot(both, to_row, precision=HIGH, preferred_element_type=jnp.float32)
    mine_ref[...] = both[:8]
    slope_rows_ref[...] = both[8:]
    group_at = group_of(lax.div(iota((count, tokens), 1), group), count, cubed)
    to_group = (group_at == iota((count, tokens), 0)).astype(jnp.float32)
    place_ref[:count] = jnp.dot(to_group, to_row, preferred_element_type=jnp.float32)
    in_group = lax.rem(iota((group, tokens), 1), group) == iota((group, tokens), 0)
    place_ref[count:] = jnp.dot(
        in_group.astype(jnp.float32), to_row, preferred_element_type=jnp.float32
    )
    if not cubed:
        parts = [ref[...].astype(jnp.float32) for ref in input_refs]
        inputs_ref[...] = jnp.concatenate(parts, axis=0).astype(jnp.bfloat16)


def final_kernel(sizes, paired, cubed, got_count, local_experts, *refs):
    got_refs, rest = refs[:got_count], refs[got_count:]
    mine_ref, slope_rows_ref, place_ref, *input_refs, slope_ref, weight_ref = rest[:-5]
    rest = rest[-5:]
    input_far, router_far, input_ref, router_ref, sems = rest
    group, expert_total, _, _ = sizes
    tokens = slope_ref.shape[0]
    count = tokens // group
    share = router_ref.shape[1]
    dp_me, me = lax.axis_index("dp"), lax.axis_index("expert")
    if cubed:
        sources = [(ref[:group], lax.bitwise_xor(me, 2 * b)) for b, ref in enumerate(got_refs)]
        parts = [
            ref[half * group : (half + 1) * group, :share].astype(jnp.float32)
            for half in (1, 2)
            for ref in got_refs
        ]
        inputs = jnp.concatenate(parts, axis=0).astype(jnp.bfloat16)
    else:
        sources = [(got_refs[0][j], j) for j in range(count)]
        inputs = input_refs[0][...]
    sums = jnp.zeros((group, 2 * count), jnp.float32)
    for got, _ in sources:
        sums = sums + got[:, share : share + 2 * count].astype(jnp.float32)
    mixture = sums[:, :count] + sums[:, count:]
    mixed = jnp.zeros((group, share), jnp.float32)
    given = jnp.zeros((group, expert_total), jnp.float32)
    part = (4 * local_experts, expert_total)
    place = lax.rem(iota(part, 0), 2 * local_experts)
    order = place_of(lax.rem(place, local_experts), dp_me, paired)
    for got, source in sources:
        mixed = mixed + got[:, :share].astype(jnp.float32)
        first = (source - lax.rem(source, 2) + lax.div(place, local_experts)) * local_experts
        to_expert = (iota(part, 1) == first + order).astype(jnp.bfloat16)
        shares = got[:, share + 2 * count : share + 2 * count + 4 * local_experts]
        given = given + jnp.dot(shares, to_expert, preferred_element_type=jnp.float32)
    my_mixture = jnp.sum(
        jnp.where(iota((group, count), 1) == me, mixture, 0.0), axis=1, keepdims=True
    )
    if cubed:
        my_slope = slope_ref[:group, :]
    else:
        my_slope = slope_ref[pl.ds(pl.multiple_of(me * group, group), group), :]
    my_grad = (my_slope * (route_scale * given - my_mixture)).astype(jnp.bfloat16)
    routed = jnp.dot(my_grad, weight_ref[...], preferred_element_type=jnp.float32)
    input_ref[0] = (mixed + routed).astype(jnp.bfloat16)
    store = pltpu.make_async_copy(input_ref, input_far, sems.at[0])
    store.start()
    wide = jnp.dot(
        mixture, place_ref[:count], precision=HIGH, preferred_element_type=jnp.float32
    )
    row_mixture = jnp.sum(wide * place_ref[count:], axis=0, keepdims=True)
    lines = slope_rows_ref[...] * (mine_ref[...] - row_mixture)
    grads = jnp.dot(
        lines.astype(jnp.bfloat16), inputs, preferred_element_type=jnp.float32
    )
    for e in range(local_experts):
        place = place_of(e, dp_me, paired)
        router_ref[pl.ds(place, 1)] = grads[e : e + 1]
    last = pltpu.make_async_copy(router_ref, router_far, sems.at[1])
    last.start()
    last.wait()
    store.wait()


def local(
    grad_output,
    router_logits,
    expert_ids,
    router_input,
    router_weight,
    gate_weight,
    up_weight,
    down_weight,
    gate_saved,
    up_saved,
):
    expert_count, dp_count = lax.axis_size("expert"), lax.axis_size("dp")
    _, group, share = grad_output.shape
    expert_total = router_logits.shape[2]
    top = expert_ids.shape[2]
    local_experts, slots, hidden_size = gate_saved.shape
    depth = slots // expert_count
    rows = local_experts * slots
    piece = rows // dp_count
    tokens = expert_count * group
    aux = -(-(3 * expert_total + top) // LANES) * LANES
    bf16, f32 = jnp.bfloat16, jnp.float32
    paired = dp_count == local_experts and dp_count & (dp_count - 1) == 0
    cubed = paired and dp_count == 4 and expert_count == 8
    sizes = (group, expert_total, top, depth)
    own_tokens = router_input.shape[1]

    def swap(value, axis, k):
        count = lax.axis_size(axis)
        return lax.ppermute(value, axis, [(j, j ^ k) for j in range(count)])

    def cross(value, k):
        there = [(d ^ k) * expert_count + (e ^ 1) for d in range(dp_count) for e in range(expert_count)]
        return lax.ppermute(value, ("dp", "expert"), list(enumerate(there)))

    def gather(value):
        if not cubed:
            return [lax.all_gather(value, "expert", axis=0, tiled=True)]
        parts = [value] + [swap(value, "expert", k) for k in (3, 5, 7)]
        joined = jnp.concatenate(parts, axis=0)
        return parts + [swap(joined, "expert", 1)]

    if cubed:
        pack_shapes = ((group, aux + share),) + tuple((n * own_tokens, share) for n in (1, 2, 1))
    else:
        pack_shapes = ((2 * group, aux + share),)
    packed, *pieces = call(
        functools.partial(pack_kernel, expert_total, cubed),
        tuple((shape, bf16) for shape in pack_shapes),
        (router_logits, expert_ids, grad_output, router_input),
        scratch=(
            VMEM(router_logits.shape, f32),
            VMEM(expert_ids.shape, jnp.int32),
            VMEM(grad_output.shape, bf16),
            VMEM(router_input.shape, bf16),
            pltpu.SemaphoreType.DMA((4,)),
        ),
        far_args=True,
    )
    packed = call(keep_kernel, (packed.shape, bf16), (packed,), flops=4 * 10**10)
    if cubed:
        pieces[1] = swap(pieces[1], "dp", 1)
    token_parts = gather(packed)
    sends = call(
        functools.partial(down_kernel, sizes, aux, paired, cubed, len(token_parts)),
        (((slots, hidden_size), bf16),) * local_experts,
        (*token_parts, down_weight.swapaxes(1, 2)),
        scratch=(VMEM((2, tokens, hidden_size), bf16),),
    )
    if cubed:
        parts = [cross(sends[k], k) for k in range(dp_count)]
    elif paired:
        parts = [sends[0]] + [swap(sends[k], "dp", k) for k in range(1, dp_count)]
    else:
        all_sends = jnp.concatenate(sends, axis=0).reshape(dp_count, piece, hidden_size)
        parts = list(lax.all_to_all(all_sends, "dp", 0, 0, tiled=True))
    if cubed:
        piece_shape = (2 * own_tokens, share)
    else:
        piece_shape = (dp_count, expert_count * own_tokens, share)
    full, slope, piece_out = call(
        functools.partial(table_kernel, sizes, aux, local_experts, paired, cubed, len(token_parts)),
        (((tokens, rows), f32), ((tokens, expert_total), f32), (piece_shape, bf16)),
        (*token_parts, *((pieces[2], pieces[1]) if cubed else ())),
    )
    if cubed:
        pieces = [pieces[0], pieces[1], swap(piece_out, "dp", 2)]
    else:
        pieces = list(lax.all_to_all(piece_out, "dp", 0, 0, tiled=True))
    hidden = sum(part.astype(f32) for part in parts).astype(bf16)
    if cubed:
        blocks = [cross(hidden, k) for k in range(dp_count)]
    elif paired:
        blocks = [hidden] + [swap(hidden, "dp", k) for k in range(1, dp_count)]
    else:
        spread = lax.all_gather(hidden, "dp", axis=0, tiled=True)
        blocks = list(spread.reshape(local_experts, slots, hidden_size))

    weights = (gate_weight, up_weight, gate_saved, up_saved)
    lanes = -(-rows // LANES) * LANES
    done = []
    turns = (0, 1, 2, 3) if cubed else tuple(range(local_experts))
    for k in turns[:-1]:
        done += call(
            functools.partial(input_kernel, k, paired),
            (((slots, share), f32), ((1, lanes), f32)),
            (*weights, blocks[k]),
        )
    width = -(-(share + 2 * expert_count + 4 * local_experts) // LANES) * LANES
    if cubed:
        half = (expert_count // 2 + 1, group, width)
        mix_shapes = ((half, f32), (half, bf16))
    else:
        mix_shapes = (((expert_count, group, width), bf16),)
    *mixed, own = call(
        functools.partial(mix_kernel, turns, group, paired, cubed),
        (*mix_shapes, ((tokens, LANES), f32)),
        (full, *weights, blocks[turns[-1]], *(pieces if cubed else ()), *done),
        scratch=(VMEM((rows, share), f32), VMEM((1, lanes), f32)),
    )
    if cubed:
        far = swap(mixed[1], "expert", 1)
        sums = call(
            functools.partial(pair_kernel, share, expert_count, local_experts),
            (((3 * group, width), bf16),) * (expert_count // 2),
            (mixed[0], far),
        )
        got = [sums[0]] + [swap(sums[k], "expert", 2 * k) for k in (1, 2, 3)]
    else:
        got = [lax.all_to_all(mixed[0], "expert", 0, 0, tiled=True)]
    ready = call(
        functools.partial(ready_kernel, sizes, paired, cubed),
        (
            ((8, tokens), f32),
            ((8, tokens), f32),
            ((expert_count + group, tokens), f32),
            *(() if cubed else (((tokens, share), bf16),)),
        ),
        (own, slope, *(() if cubed else pieces)),
    )
    grad_input, grad_router = call(
        functools.partial(final_kernel, sizes, paired, cubed, len(got), local_experts),
        (((1, group, share), bf16), ((local_experts, share), f32)),
        (*got, *ready, slope, router_weight),
        scratch=(
            VMEM((1, group, share), bf16),
            VMEM((local_experts, share), f32),
            pltpu.SemaphoreType.DMA((2,)),
        ),
        far_outs=True,
    )
    return grad_input, grad_router


def solution(mesh):
    placed = (
        P("expert", None, "dp"),
        P("expert", None, None),
        P("expert", None, None),
        P("expert", "dp", None),
        P(None, "dp"),
        P("expert", "dp", None),
        P("expert", "dp", None),
        P("expert", None, "dp"),
        P("expert", None, None),
        P("expert", None, None),
    )

    return jax.shard_map(
        local,
        mesh=mesh,
        in_specs=placed,
        out_specs=(P("expert", None, "dp"), P("expert", "dp")),
        check_vma=False,
    )
```
